128 devices in a mesh: section: 32 (over y, z, core), state: 4 (over x).
Axes of the slice: x: 4, y: 4, z: 4, core: 2. Of those that a mesh axis runs over, the one named last changes fastest.
Arguments:
- initial_state: float32 [32, 1024], P('state'), may hold values from -6 to 6
- state_ref: float32 [768, 32, 1024], P('section', 'state'), may hold values from -6 to 6
- state_weight: float32 [768, 32, 1024], P('section', 'state'), may hold values from 0.2 to 5
- input_matrix: bfloat16 [32, 1024, 512], P('state'), may hold values from -0.25 to 0.25
- kkt_inverse: float32 [512, 512], replicated, may hold values from -1 to 1, as said below
- input_bound: float32 [512], replicated, may hold values from 0.02 to 0.3
Outputs:
- states: float32 [768, 32, 1024], P('section', 'state')
- boxed: float32 [768, 512], P('section')
- dual_vars: float32 [768, 32, 1024], P('section', 'state')
- history: float32 [10, 2], replicated
The draws below stay inside these ranges and needn't reach their ends.
Inputs may be any that keep to these rules, and one draw needn't show every extreme that they name: `kkt_inverse`: a symmetric matrix.
All inputs are finite; a program needn't handle non-finite values.
Results may differ from the reference program's by a relative error of at most 0.003.
Values may be sent and summed in bfloat16 or wider, within the bound.
A program may use at most 128 MiB of HBM per device.

```python
import math
import jax
import jax.numpy as jnp
from jax import lax

GX = 32
GY = 32
GZ = 32
NU = 512
ITERS = 10
PLANE = 1024
HORIZON = 768


def draw_kkt_inverse(key, part):
    noise_key = jax.random.fold_in(key, 7)
    noise = jax.random.normal(noise_key, (NU, NU), jnp.float32)
    symmetric = (noise + noise.T) * (0.25 / (2.0 * NU) ** 0.5)
    factor = 1.0 / (1.0 + 2.0 * GX * GY * GZ / NU)
    return factor * (jnp.eye(NU, dtype=jnp.float32) + symmetric)


def block_scale(own_key, extent, cuts, low, largest):
    gain = 1.0
    for dim, parts in cuts:
        steps = jax.random.uniform(jax.random.fold_in(jax.random.fold_in(own_key, 6), dim), (parts,), jnp.float32, low / len(cuts), largest / len(cuts))
        gain = gain * jnp.repeat(jnp.exp(steps), extent[dim] // parts).reshape((-1,) + (1,) * (len(extent) - 1 - dim))
    return gain


def bell_draw(own_key, extent, width, bound, split=(), kind=jnp.bfloat16):
    array = width * jax.random.normal(own_key, extent, jnp.float32)
    if split:
        array = array * block_scale(own_key, extent, split, -0.22, 0.18)
    return jnp.clip(array, -bound, bound).astype(kind)


def setup_inputs(seed: int = 0) -> dict:
    seeds = jax.random.split(jax.random.key(seed), 7)
    return {
        "initial_state": bell_draw(seeds[0], (GX, PLANE), 1.0, 6.0, ((0, 4),), jnp.float32),
        "state_ref": bell_draw(seeds[1], (HORIZON, GX, PLANE), 1.0, 6.0, ((0, 32), (1, 4)), jnp.float32),
        "state_weight": jnp.clip(jnp.exp(math.log(5.0) - 3.218876 * jax.random.uniform(seeds[2], (HORIZON, GX, PLANE), jnp.float32) ** block_scale(seeds[2], (HORIZON, GX, PLANE), ((0, 32), (1, 4)), -0.2, 0.2)), 0.2, 5.0),
        "input_matrix": bell_draw(seeds[3], (GX, PLANE, NU), NU ** -0.5, 0.25, ((0, 4),)),
        "kkt_inverse": draw_kkt_inverse(jax.random.fold_in(seeds[6], 71), 0),
        "input_bound": jnp.clip(jnp.exp(jax.random.uniform(seeds[5], (NU,), jnp.float32, math.log(0.02), math.log(0.3))), 0.02, 0.3),
    }


diffusion = 0.15
epsilon = 1e-06

def stencil(padded):
    centre = padded[:, 1:-1]
    across = padded[:, 2:] + padded[:, :-2]
    depth = centre.shape[-1]
    flat_pad = jnp.pad(centre, ((0, 0), (0, 0), (GZ, GZ)))
    along_y = flat_pad[:, :, 2 * GZ:] + flat_pad[:, :, :-2 * GZ]
    lower_z = jnp.pad(centre, ((0, 0), (0, 0), (1, 0)))[:, :, :-1]
    upper_z = jnp.pad(centre, ((0, 0), (0, 0), (0, 1)))[:, :, 1:]
    z_index = jnp.arange(depth) % GZ
    along_z = jnp.where(z_index > 0, lower_z, 0.0) + jnp.where(z_index < GZ - 1, upper_z, 0.0)
    return centre + diffusion * (across + along_y + along_z - 6.0 * centre)

def reference(initial_state, state_ref, state_weight, input_matrix, kkt_inverse, input_bound):
    horizon = state_ref.shape[0]
    cell_total = input_matrix.shape[0] * input_matrix.shape[1]
    input_width = input_matrix.shape[2]
    matrix = input_matrix.reshape(cell_total, input_width)
    penalty = float(cell_total) / input_width
    states = jnp.zeros_like(state_ref)
    dual_vars = jnp.zeros_like(state_ref)
    boxed = jnp.zeros((horizon, input_width), jnp.float32)
    scaled = jnp.zeros((horizon, input_width), jnp.float32)
    history = []
    for iteration in range(ITERS):
        before = jnp.concatenate([initial_state[None], states[:-1]], 0)
        moved_prior = stencil(jnp.pad(before, ((0, 0), (1, 1), (0, 0))))
        target = states - moved_prior + dual_vars
        target_low = target.astype(jnp.bfloat16).reshape(horizon, cell_total)
        pulled = jnp.dot(target_low, matrix, preferred_element_type=jnp.float32)
        rhs_rows = pulled + penalty * (boxed - scaled)
        inputs = jnp.dot(rhs_rows, kkt_inverse, precision=lax.Precision.HIGHEST)
        inputs_low = inputs.astype(jnp.bfloat16)
        driven = jnp.dot(inputs_low, matrix.T, preferred_element_type=jnp.float32).reshape(states.shape)
        defect = target - driven
        ahead_defect = jnp.concatenate([defect[1:], jnp.zeros_like(defect[:1])], 0)
        back_term = stencil(jnp.pad(ahead_defect, ((0, 0), (1, 1), (0, 0))))
        updated = (state_weight * state_ref + (states - defect) + back_term + states) / (state_weight + 2.0)
        primal = updated - moved_prior - driven
        dual_vars = dual_vars + primal
        boxed_new = jnp.clip(inputs + scaled, -input_bound, input_bound)
        box_gap = inputs - boxed_new
        scaled = scaled + box_gap
        boxed = boxed_new
        states = updated
        history.append(jnp.stack([jnp.sqrt(jnp.mean(primal * primal) + epsilon), jnp.sqrt(jnp.mean(box_gap * box_gap) + epsilon)]))
    return (states, boxed, dual_vars, jnp.stack(history))
```

```python
import functools

import jax
import jax.numpy as jnp
from jax import lax
from jax.experimental import pallas as pl
from jax.experimental.pallas import tpu as pltpu
from jax.sharding import PartitionSpec as P

GX = 32
GY = 32
GZ = 32
ITERS = 10
PLANES = 8
CHUNKS = 8
ROWS = 24
LANES = 128
WIDTH = 512
PLANE = 1024
diffusion = 0.15
epsilon = 1e-06
MESH = pl.DeviceIdType.MESH
F32 = jnp.float32
BF16 = jnp.bfloat16


def in_plane(chunks, across):
    lane = lax.broadcasted_iota(jnp.int32, (1, LANES), 1)
    along = lane % GZ
    down = [pltpu.roll(c, GZ, 1) for c in chunks]
    up = [pltpu.roll(c, LANES - GZ, 1) for c in chunks]
    out = []
    for j, c in enumerate(chunks):
        below = down[j - 1] if j > 0 else 0.0
        above = up[j + 1] if j < CHUNKS - 1 else 0.0
        y_sum = jnp.where(lane < GZ, below, down[j]) + jnp.where(lane >= LANES - GZ, above, up[j])
        lower = jnp.where(along > 0, pltpu.roll(c, 1, 1), 0.0)
        upper = jnp.where(along < GZ - 1, pltpu.roll(c, LANES - 1, 1), 0.0)
        total = y_sum + lower + upper
        if across is not None:
            total = total + across[j]
        out.append((1.0 - 6.0 * diffusion) * c + diffusion * total)
    return out


def kernel(sections, groups, init_ref, ref_hbm, weight_hbm, matrix_hbm, kkt_ref, bound_ref,
           states_out, boxed_out, dual_out, hist_out,
           ref_ref, weight_ref, mat, mat_t, S, AS, T, D, dual, wref, recip, lhs, halo,
           send24, send0, own24, low24, high24, own0, low0, high0,
           part, part_in, tile, tile_prev, tile_next, k_high, k_low, pul, boxed, scaled,
           hist, first_in, second, second_in,
           load_sem, flat_sem, halo_send, halo_recv, send_sem, recv_sem, hist_send, hist_recv):
    s = lax.axis_index("section")
    x = lax.axis_index("state")
    columns = sections // 2

    def inside(ds, dx):
        return (s + ds >= 0) & (s + ds < sections) & (x + dx >= 0) & (x + dx < groups)

    def rotated(d):
        return lax.rem(x + d, groups)

    pair_count = 2 * groups

    def pair_peer(e):
        flat = lax.rem(lax.rem(s, 2) * groups + x + e, pair_count)
        return (s - lax.rem(s, 2) + flat // groups, lax.rem(flat, groups))

    def column_peer(e):
        return (lax.rem(s // 2 + e, columns) * 2 + lax.rem(s, 2), x)

    zeros = lambda ref: ref.__setitem__(Ellipsis, jnp.zeros(ref.shape, ref.dtype))
    for ref in (halo, own24, low24, high24, own0, low0, high0):
        zeros(ref)

    barrier = pltpu.get_barrier_semaphore()

    def greet(target):
        pl.semaphore_signal(barrier, inc=1, device_id=target, device_id_type=MESH)

    for d in range(1, groups):
        greet((s, rotated(d)))
    for d in range(groups):
        @pl.when(s > 0)
        def _():
            greet((s - 1, rotated(d)))

        @pl.when(s < sections - 1)
        def _():
            greet((s + 1, rotated(d)))
    for e in range(1, columns):
        greet(column_peer(e))

    loads = [pltpu.make_async_copy(matrix_hbm.at[p], mat.at[p + 1], load_sem.at[p]) for p in range(PLANES)]
    flat_loads = []
    for j in range(CHUNKS):
        cells = pl.ds(j * LANES, LANES)
        flat_loads.append(pltpu.make_async_copy(weight_hbm.at[:, cells], weight_ref.at[j], flat_sem.at[0, j]))
        flat_loads.append(pltpu.make_async_copy(ref_hbm.at[:, cells], ref_ref.at[j], flat_sem.at[1, j]))
    for copy in flat_loads + loads:
        copy.start()

    for ref in (AS, T, D, dual, S, boxed, scaled, hist):
        zeros(ref)

    @pl.when(x == 0)
    def _():
        mat[0] = jnp.zeros((PLANE, WIDTH), BF16)

    @pl.when(x == groups - 1)
    def _():
        mat[PLANES + 1] = jnp.zeros((PLANE, WIDTH), BF16)

    neighbours = (
        (s > 0).astype(jnp.int32) * groups
        + (s < sections - 1).astype(jnp.int32) * groups
        + (groups - 1)
        + (columns - 1)
    )
    pl.semaphore_wait(barrier, neighbours)

    def plane_copy(side):
        source = 0 if side == 0 else PLANES - 1
        target = PLANES + 1 if side == 0 else 0
        return pltpu.make_async_remote_copy(
            src_ref=matrix_hbm.at[source], dst_ref=mat.at[target],
            send_sem=halo_send.at[side], recv_sem=halo_recv.at[side],
            device_id=(s, x - 1 if side == 0 else x + 1), device_id_type=MESH)

    @pl.when(x > 0)
    def _():
        plane_copy(0).start()

    @pl.when(x < groups - 1)
    def _():
        plane_copy(1).start()

    kkt = kkt_ref[...]
    high = kkt.astype(BF16)
    k_high[...] = high
    k_low[...] = (kkt - high.astype(F32)).astype(BF16)

    for copy in flat_loads:
        copy.wait()
    for p in range(PLANES):
        for j in range(CHUNKS):
            weight = weight_ref[j, pl.ds(p, ROWS, stride=PLANES), :]
            wref[p, j] = weight * ref_ref[j, pl.ds(p, ROWS, stride=PLANES), :]
            recip[p, j] = 1.0 / (weight + 2.0)

    @pl.when(s == 0)
    def _():
        for p in range(PLANES):
            own = [init_ref[p:p + 1, j * LANES:(j + 1) * LANES] for j in range(CHUNKS)]
            across = []
            for j in range(CHUNKS):
                cells = slice(j * LANES, (j + 1) * LANES)
                total = jnp.zeros((1, LANES), F32)
                if p > 0:
                    total = total + init_ref[p - 1:p, cells]
                if p < PLANES - 1:
                    total = total + init_ref[p + 1:p + 2, cells]
                across.append(total)
            moved = in_plane(own, across)
            for j in range(CHUNKS):
                AS[p, j, 7:8, :] = moved[j]
                if p in (0, PLANES - 1):
                    S[p + 1, j, 7:8, :] = own[j]

    for copy in loads:
        copy.wait()

    @pl.when(x < groups - 1)
    def _():
        plane_copy(0).wait_recv()

    @pl.when(x > 0)
    def _():
        plane_copy(1).wait_recv()

    @pl.when(x > 0)
    def _():
        plane_copy(0).wait_send()

    @pl.when(x < groups - 1)
    def _():
        plane_copy(1).wait_send()

    def turn(p, carry):
        mat_t[p] = mat[p].T
        return carry

    lax.fori_loop(0, PLANES + 2, turn, 0)

    penalty = float(GX * GY * GZ) / WIDTH
    not_last = jnp.where(s < sections - 1, 1.0, 0.0).astype(F32)
    cross = [(0, -1), (0, 1), (1, 0), (1, 1), (1, -1), (-1, 0), (-1, 1), (-1, -1)]
    base_index = len(cross)

    def messages(slot):
        side = 2 * PLANE
        sources = [
            (lhs.at[:, pl.ds(0, side)], halo.at[slot, 1]),
            (lhs.at[:, pl.ds(PLANES * PLANE, side)], halo.at[slot, 0]),
            (send24.at[pl.ds(1, PLANES)], own24.at[slot]),
            (send24.at[PLANES + 1], low24.at[slot]),
            (send24.at[0], high24.at[slot]),
            (send0, own0.at[slot]),
            (send0.at[PLANES - 1], low0.at[slot]),
            (send0.at[0], high0.at[slot]),
        ]
        return sources

    def cross_copy(i, slot):
        ds, dx = cross[i]
        source, target = messages(slot)[i]
        return pltpu.make_async_remote_copy(
            src_ref=source, dst_ref=target, send_sem=send_sem.at[i], recv_sem=recv_sem.at[slot, i],
            device_id=(s + ds, x + dx), device_id_type=MESH)

    def peer_copy(d, slot):
        i = base_index + d - 1
        return pltpu.make_async_remote_copy(
            src_ref=part, dst_ref=part_in.at[slot, d - 1], send_sem=send_sem.at[i],
            recv_sem=recv_sem.at[slot, i], device_id=(s, rotated(d)), device_id_type=MESH)

    def tile_copy(ds, d, slot):
        i = base_index + groups - 1 + (groups if ds > 0 else 0) + d
        target = tile_prev if ds > 0 else tile_next
        return pltpu.make_async_remote_copy(
            src_ref=tile, dst_ref=target.at[slot, d], send_sem=send_sem.at[i],
            recv_sem=recv_sem.at[slot, i], device_id=(s + ds, rotated(d)), device_id_type=MESH)

    def iteration(k, carry):
        slot = lax.rem(k, 2)

        def apply(p, c):
            chunks = [S[p + 1, j, 8:32, :] for j in range(CHUNKS)]
            across = [S[p, j, 8:32, :] + S[p + 2, j, 8:32, :] for j in range(CHUNKS)]
            for j, value in enumerate(in_plane(chunks, across)):
                AS[p, j, 8:32, :] = value
            for j in range(CHUNKS):
                moved = AS[p, j, pl.ds(7, ROWS), :]
                tail = -AS[p, j, pl.ds(31, 8), :]
                body = chunks[j] + dual[p, j] - moved
                T[p + 1, j, 0:24, :] = body
                T[p + 1, j, 24:32, :] = tail
                full = jnp.concatenate([body, tail], 0)
                lhs[:, pl.ds(pl.multiple_of((p + 1) * PLANE, PLANE) + j * LANES, LANES)] = full.astype(BF16)
                send24[p + 1, j:j + 1, :] = tail[0:1]
                send0[p, j:j + 1, :] = body[0:1]
            return c

        lax.fori_loop(0, PLANES, apply, 0)
        for p, q in ((0, 1), (PLANES + 1, PLANES)):
            for j in range(CHUNKS):
                full = -diffusion * S[q, j, pl.ds(7, 32), :]
                T[p, j] = full
                lhs[:, pl.ds(p * PLANE + j * LANES, LANES)] = full.astype(BF16)
                send24[p, j:j + 1, :] = full[24:25]

        for i, (ds, dx) in enumerate(cross):
            @pl.when(inside(ds, dx))
            def _():
                cross_copy(i, slot).start()

        part[...] = jnp.dot(lhs[...], mat[...].reshape((PLANES + 2) * PLANE, WIDTH), preferred_element_type=F32)
        for c in range(4):
            cells = slice(c * LANES, (c + 1) * LANES)
            tile[c:c + 1, :] = part[0:1, cells]
            tile[c + 4:c + 5, :] = part[24:25, cells]
        for d in range(1, groups):
            peer_copy(d, slot).start()
        for d in range(groups):
            @pl.when(s < sections - 1)
            def _():
                tile_copy(1, d, slot).start()

            @pl.when(s > 0)
            def _():
                tile_copy(-1, d, slot).start()

        for i, (ds, dx) in enumerate(cross):
            @pl.when(inside(-ds, -dx))
            def _():
                cross_copy(i, slot).wait_recv()

        for j in range(CHUNKS):
            low = slice(j * LANES, (j + 1) * LANES)
            high_ = slice(PLANE + j * LANES, PLANE + (j + 1) * LANES)
            T[1, j] = T[1, j] + halo[slot, 0, :, high_].astype(F32)
            T[PLANES, j] = T[PLANES, j] + halo[slot, 1, :, low].astype(F32)
            T[0, j] = T[0, j] + halo[slot, 0, :, low].astype(F32)
            T[PLANES + 1, j] = T[PLANES + 1, j] + halo[slot, 1, :, high_].astype(F32)
            T[0, j, 24:25, :] += low0[slot, j:j + 1, :]
            T[PLANES + 1, j, 24:25, :] += high0[slot, j:j + 1, :]
            T[1, j, 0:1, :] += low24[slot, j:j + 1, :]
            T[PLANES, j, 0:1, :] += high24[slot, j:j + 1, :]

        def complete(p, c):
            for j in range(CHUNKS):
                T[p + 1, j, 0:1, :] += own24[slot, p, j:j + 1, :]
                T[p + 1, j, 24:25, :] += own0[slot, p, j:j + 1, :]
            return c

        lax.fori_loop(0, PLANES, complete, 0)

        for d in range(1, groups):
            peer_copy(d, slot).wait_recv()
        for d in range(groups):
            @pl.when(s > 0)
            def _():
                tile_copy(1, d, slot).wait_recv()

            @pl.when(s < sections - 1)
            def _():
                tile_copy(-1, d, slot).wait_recv()

        total = part[...]
        for d in range(1, groups):
            total = total + part_in[slot, d - 1]
        pul[...] = total + penalty * (boxed[...] - scaled[...])

        @pl.when(s > 0)
        def _():
            incoming = tile_prev[slot, 0]
            for d in range(1, groups):
                incoming = incoming + tile_prev[slot, d]
            for c in range(4):
                cells = slice(c * LANES, (c + 1) * LANES)
                pul[0:1, cells] += incoming[c + 4:c + 5]

        @pl.when(s < sections - 1)
        def _():
            incoming = tile_next[slot, 0]
            for d in range(1, groups):
                incoming = incoming + tile_next[slot, d]
            for c in range(4):
                cells = slice(c * LANES, (c + 1) * LANES)
                pul[24:25, cells] += incoming[c:c + 1]

        rhs = pul[...]
        rhs_high = rhs.astype(BF16)
        rhs_low = (rhs - rhs_high.astype(F32)).astype(BF16)
        stacked = jnp.dot(jnp.concatenate([rhs_high, rhs_low], 0), k_high[...], preferred_element_type=F32)
        inputs = stacked[0:32] + stacked[32:64] + jnp.dot(rhs_high, k_low[...], preferred_element_type=F32)
        bound = bound_ref[...]
        boxed_new = jnp.clip(inputs + scaled[...], -bound, bound)
        gap = inputs - boxed_new
        scaled[...] = scaled[...] + gap
        boxed[...] = boxed_new
        inputs_low = inputs.astype(BF16)
        gap_sum = jnp.sum(gap[0:ROWS] * gap[0:ROWS], axis=(0, 1), keepdims=True)

        def drive(p, c):
            driven = jnp.dot(inputs_low, mat_t[p], preferred_element_type=F32)
            for j in range(CHUNKS):
                piece = driven[:, j * LANES:(j + 1) * LANES]
                D[p, j, 0:24, :] = T[p, j, 0:24, :] - piece[0:24]
                D[p, j, 24:32, :] = (T[p, j, 24:32, :] - piece[24:32]) * not_last
            return c

        lax.fori_loop(1, PLANES + 1, drive, 0)

        @pl.when(x > 0)
        def _():
            drive(0, 0)

        @pl.when(x < groups - 1)
        def _():
            drive(PLANES + 1, 0)

        def update(p, acc):
            chunks = [D[p + 1, j, pl.ds(1, ROWS), :] for j in range(CHUNKS)]
            across = [D[p, j, pl.ds(1, ROWS), :] + D[p + 2, j, pl.ds(1, ROWS), :] for j in range(CHUNKS)]
            back = in_plane(chunks, across)
            for j in range(CHUNKS):
                old = S[p + 1, j, 8:32, :]
                defect = D[p + 1, j, 0:24, :]
                fresh = (wref[p, j] + (2.0 * old - defect) + back[j]) * recip[p, j]
                old_dual = dual[p, j]
                new_dual = fresh - old + defect
                primal = new_dual - old_dual
                S[p + 1, j, 8:32, :] = fresh
                dual[p, j] = new_dual
                square = primal * primal
                acc = acc + (square[0:8] + square[8:16] + square[16:24])
            return acc

        acc = lax.fori_loop(0, PLANES, update, jnp.zeros((8, LANES), F32))
        primal_sum = jnp.sum(acc, axis=(0, 1), keepdims=True)
        row = lax.broadcasted_iota(jnp.int32, (8, LANES), 0)
        column = lax.broadcasted_iota(jnp.int32, (8, LANES), 1)
        hist[...] += jnp.where((column == k) & (row == 0), primal_sum, 0.0) + jnp.where(
            (column == k) & (row == 1), gap_sum, 0.0)

        for i, (ds, dx) in enumerate(cross):
            @pl.when(inside(ds, dx))
            def _():
                cross_copy(i, slot).wait_send()
        for d in range(1, groups):
            peer_copy(d, slot).wait_send()
        for d in range(groups):
            @pl.when(s < sections - 1)
            def _():
                tile_copy(1, d, slot).wait_send()

            @pl.when(s > 0)
            def _():
                tile_copy(-1, d, slot).wait_send()
        return carry

    lax.fori_loop(0, ITERS, iteration, 0)

    def first_copy(e):
        return pltpu.make_async_remote_copy(
            src_ref=hist, dst_ref=first_in.at[e - 1], send_sem=hist_send.at[e - 1], recv_sem=hist_recv.at[e - 1],
            device_id=pair_peer(e), device_id_type=MESH)

    def second_copy(e):
        i = pair_count - 2 + e
        return pltpu.make_async_remote_copy(
            src_ref=second, dst_ref=second_in.at[e - 1], send_sem=hist_send.at[i], recv_sem=hist_recv.at[i],
            device_id=column_peer(e), device_id_type=MESH)

    for e in range(1, pair_count):
        first_copy(e).start()

    for p in range(PLANES):
        for j in range(CHUNKS):
            ref_ref[j, pl.ds(p, ROWS, stride=PLANES), :] = S[p + 1, j, 8:32, :]
            weight_ref[j, pl.ds(p, ROWS, stride=PLANES), :] = dual[p, j]
    stores = []
    for j in range(CHUNKS):
        cells = pl.ds(j * LANES, LANES)
        stores.append(pltpu.make_async_copy(ref_ref.at[j], states_out.at[:, cells], flat_sem.at[0, j]))
        stores.append(pltpu.make_async_copy(weight_ref.at[j], dual_out.at[:, cells], flat_sem.at[1, j]))
    for copy in stores:
        copy.start()
    boxed_out[...] = boxed[0:ROWS]

    for e in range(1, pair_count):
        first_copy(e).wait()
    total = hist[...]
    for e in range(1, pair_count):
        total = total + first_in[e - 1]
    second[...] = total
    for e in range(1, columns):
        second_copy(e).start()
    for e in range(1, columns):
        second_copy(e).wait()
    for e in range(1, columns):
        total = total + second_in[e - 1]
    row = lax.broadcasted_iota(jnp.int32, (8, LANES), 0)
    cells = float(ROWS * sections * GX * GY * GZ)
    inputs_count = float(ROWS * sections * WIDTH * groups)
    for copy in stores:
        copy.wait()
    hist_out[...] = jnp.sqrt(jnp.where(row == 0, total * (1.0 / cells), total * (1.0 / inputs_count)) + epsilon)


def solution(mesh):
    sections, groups = mesh.shape["section"], mesh.shape["state"]
    columns = sections // 2

    def local(initial_state, state_ref, state_weight, input_matrix, kkt_inverse, input_bound):
        vmem = pl.BlockSpec(memory_space=pltpu.VMEM)
        any_space = pl.BlockSpec(memory_space=pl.ANY)
        flat = (ROWS * PLANES, PLANE)
        V = pltpu.VMEM
        DMA = pltpu.SemaphoreType.DMA
        message_count = 8 + groups - 1 + 2 * groups
        compact = (CHUNKS, LANES)
        states, boxed, dual_vars, record = pl.pallas_call(
            functools.partial(kernel, sections, groups),
            out_shape=(
                jax.ShapeDtypeStruct(flat, F32),
                jax.ShapeDtypeStruct((ROWS, WIDTH), F32),
                jax.ShapeDtypeStruct(flat, F32),
                jax.ShapeDtypeStruct((8, LANES), F32),
            ),
            in_specs=[vmem, any_space, any_space, any_space, vmem, vmem],
            out_specs=(any_space, vmem, any_space, vmem),
            scratch_shapes=[
                V((CHUNKS, ROWS * PLANES, LANES), F32),
                V((CHUNKS, ROWS * PLANES, LANES), F32),
                V((PLANES + 2, PLANE, WIDTH), BF16),
                V((PLANES + 2, WIDTH, PLANE), BF16),
                V((PLANES + 2, CHUNKS, 40, LANES), F32),
                V((PLANES, CHUNKS, 40, LANES), F32),
                V((PLANES + 2, CHUNKS, 32, LANES), F32),
                V((PLANES + 2, CHUNKS, 32, LANES), F32),
                V((PLANES, CHUNKS, ROWS, LANES), F32),
                V((PLANES, CHUNKS, ROWS, LANES), F32),
                V((PLANES, CHUNKS, ROWS, LANES), F32),
                V((32, (PLANES + 2) * PLANE), BF16),
                V((2, 2, 32, 2 * PLANE), BF16),
                V((PLANES + 2, *compact), F32),
                V((PLANES, *compact), F32),
                V((2, PLANES, *compact), F32),
                V((2, *compact), F32),
                V((2, *compact), F32),
                V((2, PLANES, *compact), F32),
                V((2, *compact), F32),
                V((2, *compact), F32),
                V((32, WIDTH), F32),
                V((2, groups - 1, 32, WIDTH), F32),
                V(compact, F32),
                V((2, groups, *compact), F32),
                V((2, groups, *compact), F32),
                V((WIDTH, WIDTH), BF16),
                V((WIDTH, WIDTH), BF16),
                V((32, WIDTH), F32),
                V((32, WIDTH), F32),
                V((32, WIDTH), F32),
                V(compact, F32),
                V((2 * groups - 1, *compact), F32),
                V(compact, F32),
                V((max(columns - 1, 1), *compact), F32),
                DMA((PLANES,)),
                DMA((2, CHUNKS)),
                DMA((2,)),
                DMA((2,)),
                DMA((message_count,)),
                DMA((2, message_count)),
                DMA((2 * groups + columns,)),
                DMA((2 * groups + columns,)),
            ],
            compiler_params=pltpu.CompilerParams(
                collective_id=0, has_side_effects=True, vmem_limit_bytes=64000 * 1024),
        )(
            initial_state,
            state_ref.reshape(flat),
            state_weight.reshape(flat),
            input_matrix,
            kkt_inverse,
            input_bound.reshape(1, WIDTH),
        )
        return (
            states.reshape(state_ref.shape),
            boxed,
            dual_vars.reshape(state_ref.shape),
            record[0:2, 0:ITERS].T,
        )

    return jax.shard_map(
        local,
        mesh=mesh,
        in_specs=(
            P("state", None),
            P("section", "state", None),
            P("section", "state", None),
            P("state", None, None),
            P(),
            P(),
        ),
        out_specs=(P("section", "state", None), P("section", None), P("section", "state", None), P()),
        check_vma=False,
    )
```

```python
import functools

import jax
import jax.numpy as jnp
from jax import lax
from jax.experimental import pallas as pl
from jax.experimental.pallas import tpu as pltpu
from jax.sharding import PartitionSpec as P

GX = 32
GY = 32
GZ = 32
ITERS = 10
PIECES = 4
HALO_FIRST = True
PLANES = 8
CHUNKS = 8
ROWS = 24
LANES = 128
WIDTH = 512
PLANE = 1024
diffusion = 0.15
epsilon = 1e-06
MESH = pl.DeviceIdType.MESH
F32 = jnp.float32
BF16 = jnp.bfloat16


def in_plane(chunks, across):
    lane = lax.broadcasted_iota(jnp.int32, (1, LANES), 1)
    along = lane % GZ
    down = [pltpu.roll(c, GZ, 1) for c in chunks]
    up = [pltpu.roll(c, LANES - GZ, 1) for c in chunks]
    out = []
    for j, c in enumerate(chunks):
        below = down[j - 1] if j > 0 else 0.0
        above = up[j + 1] if j < CHUNKS - 1 else 0.0
        y_sum = jnp.where(lane < GZ, below, down[j]) + jnp.where(lane >= LANES - GZ, above, up[j])
        lower = jnp.where(along > 0, pltpu.roll(c, 1, 1), 0.0)
        upper = jnp.where(along < GZ - 1, pltpu.roll(c, LANES - 1, 1), 0.0)
        total = y_sum + lower + upper
        if across is not None:
            total = total + across[j]
        out.append((1.0 - 6.0 * diffusion) * c + diffusion * total)
    return out


def kernel(sections, groups, init_ref, ref_hbm, weight_hbm, matrix_hbm, kkt_ref, bound_ref,
           states_out, boxed_out, dual_out, hist_out,
           ref_ref, weight_ref, mat, mat_t, S, AS, T, D, dual, wref, recip, lhs, halo,
           send24, send0, own24, low24, high24, own0, low0, high0,
           part, part_low, part_in, init_in, tile, tile_prev, tile_next, k_high, k_low, pul, boxed, scaled,
           hist, first_in, second, second_in,
           load_sem, flat_sem, halo_send, halo_recv, pass_send, pass_recv, init_send, init_recv, send_sem, recv_sem, hist_send, hist_recv):
    s = lax.axis_index("section")
    x = lax.axis_index("state")
    columns = sections // 2

    def inside(ds, dx):
        return (s + ds >= 0) & (s + ds < sections) & (x + dx >= 0) & (x + dx < groups)

    def rotated(d):
        return lax.rem(x + d, groups)

    pair_count = 2 * groups

    def pair_peer(e):
        flat = lax.rem(lax.rem(s, 2) * groups + x + e, pair_count)
        return (s - lax.rem(s, 2) + flat // groups, lax.rem(flat, groups))

    def column_peer(e):
        return (lax.rem(s // 2 + e, columns) * 2 + lax.rem(s, 2), x)

    zeros = lambda ref: ref.__setitem__(Ellipsis, jnp.zeros(ref.shape, ref.dtype))
    for ref in (halo, own24, low24, high24, own0, low0, high0, init_in):
        zeros(ref)

    barrier = pltpu.get_barrier_semaphore()

    def greet(target):
        pl.semaphore_signal(barrier, inc=1, device_id=target, device_id_type=MESH)

    for d in range(1, groups):
        greet((s, rotated(d)))
    for d in range(groups):
        @pl.when(s > 0)
        def _():
            greet((s - 1, rotated(d)))

        @pl.when(s < sections - 1)
        def _():
            greet((s + 1, rotated(d)))
    for e in range(1, columns):
        greet(column_peer(e))

    loads = [pltpu.make_async_copy(matrix_hbm.at[p], mat.at[p + 1], load_sem.at[p]) for p in range(PLANES)]
    flat_loads = []
    for j in range(CHUNKS):
        cells = pl.ds(j * LANES, LANES)
        flat_loads.append(pltpu.make_async_copy(weight_hbm.at[:, cells], weight_ref.at[j], flat_sem.at[0, j]))
        flat_loads.append(pltpu.make_async_copy(ref_hbm.at[:, cells], ref_ref.at[j], flat_sem.at[1, j]))
    for copy in flat_loads + loads:
        copy.start()

    for ref in (AS, T, D, dual, S, boxed, scaled, hist):
        zeros(ref)

    @pl.when(x == 0)
    def _():
        mat[0] = jnp.zeros((PLANE, WIDTH), BF16)

    @pl.when(x == groups - 1)
    def _():
        mat[PLANES + 1] = jnp.zeros((PLANE, WIDTH), BF16)

    neighbours = (
        (s > 0).astype(jnp.int32) * groups
        + (s < sections - 1).astype(jnp.int32) * groups
        + (groups - 1)
        + (columns - 1)
    )
    pl.semaphore_wait(barrier, neighbours)

    half = lax.rem(s, 2) * (PLANE // 2)
    twin = s + 1 - 2 * lax.rem(s, 2)
    depth = PLANE // 2 // PIECES

    def plane_copy(side, piece):
        source = 0 if side == 0 else PLANES - 1
        target = PLANES + 1 if side == 0 else 0
        rows = pl.ds(pl.multiple_of(half + piece * depth, depth), depth)
        return pltpu.make_async_remote_copy(
            src_ref=matrix_hbm.at[source, rows], dst_ref=mat.at[target, rows],
            send_sem=halo_send.at[side, piece], recv_sem=halo_recv.at[side, piece],
            device_id=(s, x - 1 if side == 0 else x + 1), device_id_type=MESH)

    def pass_copy(side, piece, start):
        target = PLANES + 1 if side == 0 else 0
        rows = pl.ds(pl.multiple_of(start + piece * depth, depth), depth)
        return pltpu.make_async_remote_copy(
            src_ref=mat.at[target, rows], dst_ref=mat.at[target, rows],
            send_sem=pass_send.at[side, piece], recv_sem=pass_recv.at[side, piece],
            device_id=(twin, x), device_id_type=MESH)

    sends_to = (x > 0, x < groups - 1)
    gets_from = (x < groups - 1, x > 0)

    def init_copy(side):
        return pltpu.make_async_remote_copy(
            src_ref=init_ref, dst_ref=init_in.at[1 - side], send_sem=init_send.at[side],
            recv_sem=init_recv.at[side], device_id=(s, x - 1 if side == 0 else x + 1), device_id_type=MESH)

    for side in range(2):
        @pl.when((s == 0) & sends_to[side])
        def _():
            init_copy(side).start()

        @pl.when(sends_to[side])
        def _():
            for piece in range(PIECES):
                plane_copy(side, piece).start()

    kkt = kkt_ref[...]
    high = kkt.astype(BF16)
    k_high[...] = high
    k_low[...] = (kkt - high.astype(F32)).astype(BF16)

    for copy in flat_loads:
        copy.wait()
    for p in range(PLANES):
        for j in range(CHUNKS):
            weight = weight_ref[j, pl.ds(p, ROWS, stride=PLANES), :]
            wref[p, j] = weight * ref_ref[j, pl.ds(p, ROWS, stride=PLANES), :]
            recip[p, j] = 1.0 / (weight + 2.0)

    penalty = float(GX * GY * GZ) / WIDTH
    not_last = jnp.where(s < sections - 1, 1.0, 0.0).astype(F32)
    has_side = (jnp.where(x > 0, 1.0, 0.0).astype(F32), jnp.where(x < groups - 1, 1.0, 0.0).astype(F32))
    cross = [(0, -1), (0, 1), (1, 0), (1, 1), (1, -1), (-1, 0), (-1, 1), (-1, -1)]
    base_index = len(cross)

    def messages(slot):
        side = 2 * PLANE
        return [
            (lhs.at[:, pl.ds(0, side)], halo.at[slot, 1]),
            (lhs.at[:, pl.ds(PLANES * PLANE, side)], halo.at[slot, 0]),
            (send24.at[pl.ds(1, PLANES)], own24.at[slot]),
            (send24.at[PLANES + 1], low24.at[slot]),
            (send24.at[0], high24.at[slot]),
            (send0, own0.at[slot]),
            (send0.at[PLANES - 1], low0.at[slot]),
            (send0.at[0], high0.at[slot]),
        ]

    def cross_copy(i, slot):
        ds, dx = cross[i]
        source, target = messages(slot)[i]
        return pltpu.make_async_remote_copy(
            src_ref=source, dst_ref=target, send_sem=send_sem.at[i], recv_sem=recv_sem.at[slot, i],
            device_id=(s + ds, x + dx), device_id_type=MESH)

    def peer_copy(d, slot):
        i = base_index + d - 1
        return pltpu.make_async_remote_copy(
            src_ref=part_low, dst_ref=part_in.at[slot, d - 1], send_sem=send_sem.at[i],
            recv_sem=recv_sem.at[slot, i], device_id=(s, rotated(d)), device_id_type=MESH)

    def tile_copy(ds, d, slot):
        i = base_index + groups - 1 + (groups if ds > 0 else 0) + d
        target = tile_prev if ds > 0 else tile_next
        return pltpu.make_async_remote_copy(
            src_ref=tile, dst_ref=target.at[slot, d], send_sem=send_sem.at[i],
            recv_sem=recv_sem.at[slot, i], device_id=(s + ds, rotated(d)), device_id_type=MESH)

    def apply(p):
        chunks = [S[p + 1, j, 8:32, :] for j in range(CHUNKS)]
        across = [S[p, j, 8:32, :] + S[p + 2, j, 8:32, :] for j in range(CHUNKS)]
        for j, value in enumerate(in_plane(chunks, across)):
            AS[p, j, 8:32, :] = value
        for j in range(CHUNKS):
            body = chunks[j] + dual[p, j] - AS[p, j, pl.ds(7, ROWS), :]
            tail = -AS[p, j, pl.ds(31, 8), :]
            T[p + 1, j, 0:24, :] = body
            T[p + 1, j, 24:32, :] = tail
            lhs[:, (p + 1) * PLANE + j * LANES:(p + 1) * PLANE + (j + 1) * LANES] = jnp.concatenate(
                [body, tail], 0).astype(BF16)
            send24[p + 1, j:j + 1, :] = tail[0:1]
            send0[p, j:j + 1, :] = body[0:1]

    def apply_outside(side):
        p, q = ((0, 1), (PLANES + 1, PLANES))[side]
        for j in range(CHUNKS):
            full = (-diffusion * has_side[side]) * S[q, j, pl.ds(7, 32), :]
            T[p, j] = full
            lhs[:, p * PLANE + j * LANES:p * PLANE + (j + 1) * LANES] = full.astype(BF16)
            send24[p, j:j + 1, :] = full[24:25]

    def solve(k, slot):
        total = part[...]
        for d in range(1, groups):
            total = total + part_in[slot, d - 1].astype(F32)
        pul[...] = total + penalty * (boxed[...] - scaled[...])

        @pl.when((s > 0) & (k > 0))
        def _():
            incoming = tile_prev[slot, 0]
            for d in range(1, groups):
                incoming = incoming + tile_prev[slot, d]
            for c in range(4):
                cells = slice(c * LANES, (c + 1) * LANES)
                pul[0:1, cells] += incoming[c + 4:c + 5]

        @pl.when((s < sections - 1) & (k > 0))
        def _():
            incoming = tile_next[slot, 0]
            for d in range(1, groups):
                incoming = incoming + tile_next[slot, d]
            for c in range(4):
                cells = slice(c * LANES, (c + 1) * LANES)
                pul[24:25, cells] += incoming[c:c + 1]

        rhs = pul[...]
        rhs_high = rhs.astype(BF16)
        rhs_low = (rhs - rhs_high.astype(F32)).astype(BF16)
        stacked = jnp.dot(jnp.concatenate([rhs_high, rhs_low], 0), k_high[...], preferred_element_type=F32)
        inputs = stacked[0:32] + stacked[32:64] + jnp.dot(rhs_high, k_low[...], preferred_element_type=F32)
        bound = bound_ref[...]
        boxed_new = jnp.clip(inputs + scaled[...], -bound, bound)
        gap = inputs - boxed_new
        scaled[...] = scaled[...] + gap
        boxed[...] = boxed_new
        gap_sum = jnp.sum(gap[0:ROWS] * gap[0:ROWS], axis=(0, 1), keepdims=True)
        record(k, 1, gap_sum)
        return inputs.astype(BF16)

    def record(k, kind, value):
        row = lax.broadcasted_iota(jnp.int32, (16, LANES), 0)
        column = lax.broadcasted_iota(jnp.int32, (16, LANES), 1)
        hist[...] += jnp.where((column == kind) & (row == k), value, 0.0)

    def drive(p, inputs_low):
        driven = jnp.dot(inputs_low, mat_t[p], preferred_element_type=F32)
        for j in range(CHUNKS):
            piece = driven[:, j * LANES:(j + 1) * LANES]
            D[p, j, 0:24, :] = T[p, j, 0:24, :] - piece[0:24]
            D[p, j, 24:32, :] = (T[p, j, 24:32, :] - piece[24:32]) * not_last

    def update(p, acc):
        chunks = [D[p + 1, j, pl.ds(1, ROWS), :] for j in range(CHUNKS)]
        across = [D[p, j, pl.ds(1, ROWS), :] + D[p + 2, j, pl.ds(1, ROWS), :] for j in range(CHUNKS)]
        back = in_plane(chunks, across)
        for j in range(CHUNKS):
            old = S[p + 1, j, 8:32, :]
            defect = D[p + 1, j, 0:24, :]
            fresh = (wref[p, j] + (2.0 * old - defect) + back[j]) * recip[p, j]
            old_dual = dual[p, j]
            new_dual = fresh - old + defect
            primal = new_dual - old_dual
            S[p + 1, j, 8:32, :] = fresh
            dual[p, j] = new_dual
            square = primal * primal
            acc = acc + (square[0:8] + square[8:16] + square[16:24])
        return acc

    def record_primal(k, acc):
        record(k, 0, jnp.sum(acc, axis=(0, 1), keepdims=True))

    for copy in loads:
        copy.wait()

    @pl.when(s == 0)
    def _():
        for side in range(2):
            @pl.when(gets_from[side])
            def _():
                init_copy(side).wait_recv()

            @pl.when(sends_to[side])
            def _():
                init_copy(side).wait_send()
        for p in range(PLANES):
            own = [init_ref[p:p + 1, j * LANES:(j + 1) * LANES] for j in range(CHUNKS)]
            across = []
            for j in range(CHUNKS):
                cells = slice(j * LANES, (j + 1) * LANES)
                below = init_ref[p - 1:p, cells] if p > 0 else init_in[0, PLANES - 1:PLANES, cells]
                above = init_ref[p + 1:p + 2, cells] if p < PLANES - 1 else init_in[1, 0:1, cells]
                across.append(below + above)
            for j, value in enumerate(in_plane(own, across)):
                AS[p, j, 7:8, :] = value
        for p in range(PLANES):
            apply(p)
        part[...] = jnp.dot(lhs[:, PLANE:(PLANES + 1) * PLANE],
                            mat[1:PLANES + 1].reshape(PLANES * PLANE, WIDTH), preferred_element_type=F32)
        part_low[...] = part[...].astype(BF16)
        for d in range(1, groups):
            peer_copy(d, 0).start()

    def turn(p, carry):
        mat_t[p] = mat[p].T
        return carry

    lax.fori_loop(1, PLANES + 1, turn, 0)

    @pl.when(s == 0)
    def _():
        for d in range(1, groups):
            peer_copy(d, 0).wait_recv()
        inputs_low = solve(0, 0)
        for p in range(PLANES):
            drive(p + 1, inputs_low)
        for d in range(1, groups):
            peer_copy(d, 0).wait_send()

    acc = jnp.zeros((8, LANES), F32)
    for p in range(PLANES):
        acc = update(p, acc)
    record_primal(0, acc)
    for p in range(PLANES):
        apply(p)
    apply_outside(0)
    apply_outside(1)

    for piece in range(PIECES):
        for side in range(2):
            @pl.when(gets_from[side])
            def _():
                plane_copy(side, piece).wait_recv()
                pass_copy(side, piece, half).start()
    for side in range(2):
        @pl.when(gets_from[side])
        def _():
            for piece in range(PIECES):
                pass_copy(side, piece, PLANE // 2 - half).wait_recv()
            for piece in range(PIECES):
                pass_copy(side, piece, half).wait_send()

        @pl.when(sends_to[side])
        def _():
            for piece in range(PIECES):
                plane_copy(side, piece).wait_send()
    mat_t[0] = mat[0].T
    mat_t[PLANES + 1] = mat[PLANES + 1].T

    def iteration(k, carry):
        slot = lax.rem(k, 2)

        def start_cross():
            for i, (ds, dx) in enumerate(cross):
                @pl.when(inside(ds, dx))
                def _():
                    cross_copy(i, slot).start()

        if HALO_FIRST:
            start_cross()
        pulled = jnp.dot(lhs[...], mat[...].reshape((PLANES + 2) * PLANE, WIDTH), preferred_element_type=F32)
        part_low[...] = pulled.astype(BF16)
        for c in range(4):
            cells = slice(c * LANES, (c + 1) * LANES)
            tile[c:c + 1, :] = pulled[0:1, cells]
            tile[c + 4:c + 5, :] = pulled[24:25, cells]
        part[...] = pulled
        for d in range(groups):
            @pl.when(s < sections - 1)
            def _():
                tile_copy(1, d, slot).start()

            @pl.when(s > 0)
            def _():
                tile_copy(-1, d, slot).start()
        for d in range(1, groups):
            peer_copy(d, slot).start()
        if not HALO_FIRST:
            start_cross()

        for d in range(1, groups):
            peer_copy(d, slot).wait_recv()
        for d in range(groups):
            @pl.when(s > 0)
            def _():
                tile_copy(1, d, slot).wait_recv()

            @pl.when(s < sections - 1)
            def _():
                tile_copy(-1, d, slot).wait_recv()
        inputs_low = solve(k, slot)

        for i, (ds, dx) in enumerate(cross):
            @pl.when(inside(-ds, -dx))
            def _():
                cross_copy(i, slot).wait_recv()

        for j in range(CHUNKS):
            low = slice(j * LANES, (j + 1) * LANES)
            high_ = slice(PLANE + j * LANES, PLANE + (j + 1) * LANES)
            T[1, j] = T[1, j] + halo[slot, 0, :, high_].astype(F32)
            T[PLANES, j] = T[PLANES, j] + halo[slot, 1, :, low].astype(F32)
            T[0, j] = T[0, j] + halo[slot, 0, :, low].astype(F32)
            T[PLANES + 1, j] = T[PLANES + 1, j] + halo[slot, 1, :, high_].astype(F32)
            T[0, j, 24:25, :] += low0[slot, j:j + 1, :]
            T[PLANES + 1, j, 24:25, :] += high0[slot, j:j + 1, :]
            T[1, j, 0:1, :] += low24[slot, j:j + 1, :]
            T[PLANES, j, 0:1, :] += high24[slot, j:j + 1, :]
        for p in range(PLANES):
            for j in range(CHUNKS):
                T[p + 1, j, 0:1, :] += own24[slot, p, j:j + 1, :]
                T[p + 1, j, 24:25, :] += own0[slot, p, j:j + 1, :]

        for i, (ds, dx) in enumerate(cross):
            @pl.when(inside(ds, dx))
            def _():
                cross_copy(i, slot).wait_send()
        for d in range(1, groups):
            peer_copy(d, slot).wait_send()
        for d in range(groups):
            @pl.when(s < sections - 1)
            def _():
                tile_copy(1, d, slot).wait_send()

            @pl.when(s > 0)
            def _():
                tile_copy(-1, d, slot).wait_send()

        acc = jnp.zeros((8, LANES), F32)
        for q in range(PLANES + 2):
            drive(q, inputs_low)
            if q >= 2:
                acc = update(q - 2, acc)
            if q >= 3:
                apply(q - 3)
        apply(PLANES - 1)
        apply_outside(0)
        apply_outside(1)
        record_primal(k, acc)
        return carry

    lax.fori_loop(1, ITERS, iteration, 0)

    def first_copy(e):
        return pltpu.make_async_remote_copy(
            src_ref=hist, dst_ref=first_in.at[e - 1], send_sem=hist_send.at[e - 1], recv_sem=hist_recv.at[e - 1],
            device_id=pair_peer(e), device_id_type=MESH)

    def second_copy(e):
        i = pair_count - 2 + e
        return pltpu.make_async_remote_copy(
            src_ref=second, dst_ref=second_in.at[e - 1], send_sem=hist_send.at[i], recv_sem=hist_recv.at[i],
            device_id=column_peer(e), device_id_type=MESH)

    for e in range(1, pair_count):
        first_copy(e).start()

    for p in range(PLANES):
        for j in range(CHUNKS):
            ref_ref[j, pl.ds(p, ROWS, stride=PLANES), :] = S[p + 1, j, 8:32, :]
            weight_ref[j, pl.ds(p, ROWS, stride=PLANES), :] = dual[p, j]
    stores = [
        pltpu.make_async_copy(ref_ref, states_out, flat_sem.at[0, 0]),
        pltpu.make_async_copy(weight_ref, dual_out, flat_sem.at[1, 0]),
    ]
    for copy in stores:
        copy.start()
    boxed_out[...] = boxed[0:ROWS]

    for e in range(1, pair_count):
        first_copy(e).wait()
    total = hist[...]
    for e in range(1, pair_count):
        total = total + first_in[e - 1]
    second[...] = total
    for e in range(1, columns):
        second_copy(e).start()
    for e in range(1, columns):
        second_copy(e).wait()
    for e in range(1, columns):
        total = total + second_in[e - 1]
    column = lax.broadcasted_iota(jnp.int32, (16, LANES), 1)
    cells = float(ROWS * sections * GX * GY * GZ)
    inputs_count = float(ROWS * sections * WIDTH * groups)
    for copy in stores:
        copy.wait()
    hist_out[...] = jnp.sqrt(jnp.where(column == 0, total * (1.0 / cells), total * (1.0 / inputs_count)) + epsilon)


def deliver(states, boxed, dual_vars, record, states_out, boxed_out, dual_out, record_out, a, b, sem):
    loads, stores = [], []
    for i, (source, held, target) in enumerate(((states, a, states_out), (dual_vars, b, dual_out))):
        for j in range(CHUNKS):
            cells = pl.ds(j * LANES, LANES)
            loads.append(pltpu.make_async_copy(source.at[j], held.at[j], sem.at[i, j]))
            stores.append(pltpu.make_async_copy(held.at[j], target.at[:, cells], sem.at[2 + i, j]))
    for copy in loads:
        copy.start()
    boxed_out[...] = boxed[...]
    record_out[...] = record[0:ITERS, 0:2]
    for load, store in zip(loads, stores):
        load.wait()
        store.start()
    for copy in stores:
        copy.wait()


def solution(mesh):
    sections, groups = mesh.shape["section"], mesh.shape["state"]
    columns = sections // 2

    def local(initial_state, state_ref, state_weight, input_matrix, kkt_inverse, input_bound):
        vmem = pl.BlockSpec(memory_space=pltpu.VMEM)
        any_space = pl.BlockSpec(memory_space=pl.ANY)
        flat = (ROWS * PLANES, PLANE)
        chunked = (CHUNKS, ROWS * PLANES, LANES)
        V = pltpu.VMEM
        DMA = pltpu.SemaphoreType.DMA
        message_count = 8 + groups - 1 + 2 * groups
        compact = (CHUNKS, LANES)
        states, boxed, dual_vars, record = pl.pallas_call(
            functools.partial(kernel, sections, groups),
            out_shape=(
                jax.ShapeDtypeStruct(chunked, F32),
                jax.ShapeDtypeStruct((ROWS, WIDTH), F32),
                jax.ShapeDtypeStruct(chunked, F32),
                jax.ShapeDtypeStruct((16, LANES), F32),
            ),
            in_specs=[vmem, any_space, any_space, any_space, vmem, vmem],
            out_specs=(any_space, vmem, any_space, vmem),
            scratch_shapes=[
                V((CHUNKS, ROWS * PLANES, LANES), F32),
                V((CHUNKS, ROWS * PLANES, LANES), F32),
                V((PLANES + 2, PLANE, WIDTH), BF16),
                V((PLANES + 2, WIDTH, PLANE), BF16),
                V((PLANES + 2, CHUNKS, 40, LANES), F32),
                V((PLANES, CHUNKS, 40, LANES), F32),
                V((PLANES + 2, CHUNKS, 32, LANES), F32),
                V((PLANES + 2, CHUNKS, 32, LANES), F32),
                V((PLANES, CHUNKS, ROWS, LANES), F32),
                V((PLANES, CHUNKS, ROWS, LANES), F32),
                V((PLANES, CHUNKS, ROWS, LANES), F32),
                V((32, (PLANES + 2) * PLANE), BF16),
                V((2, 2, 32, 2 * PLANE), BF16),
                V((PLANES + 2, *compact), F32),
                V((PLANES, *compact), F32),
                V((2, PLANES, *compact), F32),
                V((2, *compact), F32),
                V((2, *compact), F32),
                V((2, PLANES, *compact), F32),
                V((2, *compact), F32),
                V((2, *compact), F32),
                V((32, WIDTH), F32),
                V((32, WIDTH), BF16),
                V((2, groups - 1, 32, WIDTH), BF16),
                V((2, PLANES, PLANE), F32),
                V(compact, F32),
                V((2, groups, *compact), F32),
                V((2, groups, *compact), F32),
                V((WIDTH, WIDTH), BF16),
                V((WIDTH, WIDTH), BF16),
                V((32, WIDTH), F32),
                V((32, WIDTH), F32),
                V((32, WIDTH), F32),
                V((16, LANES), F32),
                V((2 * groups - 1, 16, LANES), F32),
                V((16, LANES), F32),
                V((max(columns - 1, 1), 16, LANES), F32),
                DMA((PLANES,)),
                DMA((2, CHUNKS)),
                DMA((2, PIECES)),
                DMA((2, PIECES)),
                DMA((2, PIECES)),
                DMA((2, PIECES)),
                DMA((2,)),
                DMA((2,)),
                DMA((message_count,)),
                DMA((2, message_count)),
                DMA((2 * groups + columns,)),
                DMA((2 * groups + columns,)),
            ],
            compiler_params=pltpu.CompilerParams(
                collective_id=0, has_side_effects=True, vmem_limit_bytes=64000 * 1024),
        )(
            initial_state,
            state_ref.reshape(flat),
            state_weight.reshape(flat),
            input_matrix,
            kkt_inverse,
            input_bound.reshape(1, WIDTH),
        )
        states, boxed, dual_vars, record = pl.pallas_call(
            deliver,
            out_shape=(
                jax.ShapeDtypeStruct(flat, F32),
                jax.ShapeDtypeStruct((ROWS, WIDTH), F32),
                jax.ShapeDtypeStruct(flat, F32),
                jax.ShapeDtypeStruct((ITERS, 2), F32),
            ),
            in_specs=[any_space, vmem, any_space, vmem],
            out_specs=(any_space, vmem, any_space, vmem),
            scratch_shapes=[V(chunked, F32), V(chunked, F32), DMA((4, CHUNKS))],
        )(states, boxed, dual_vars, record)
        return (states.reshape(state_ref.shape), boxed, dual_vars.reshape(state_ref.shape), record)

    return jax.shard_map(
        local,
        mesh=mesh,
        in_specs=(
            P("state", None),
            P("section", "state", None),
            P("section", "state", None),
            P("state", None, None),
            P(),
            P(),
        ),
        out_specs=(P("section", "state", None), P("section", None), P("section", "state", None), P()),
        check_vma=False,
    )
```

```python
import functools

import jax
import jax.numpy as jnp
from jax import lax
from jax.experimental import pallas as pl
from jax.experimental.pallas import tpu as pltpu
from jax.sharding import PartitionSpec as P

GX = 32
GY = 32
GZ = 32
ITERS = 10
BLOCKS = 8
FOLD = 1536
PLANES = 8
CHUNKS = 8
ROWS = 24
LANES = 128
WIDTH = 512
PLANE = 1024
diffusion = 0.15
epsilon = 1e-06
MESH = pl.DeviceIdType.MESH
F32 = jnp.float32
BF16 = jnp.bfloat16


def in_plane(chunk, across):
    lane = lax.broadcasted_iota(jnp.int32, (1, LANES), 1)
    along = lane % GZ
    here = chunk(0)
    before = None
    for j in range(CHUNKS):
        after = chunk(j + 1) if j < CHUNKS - 1 else None
        below = pltpu.roll(before, GZ, 1) if j > 0 else 0.0
        above = pltpu.roll(after, LANES - GZ, 1) if j < CHUNKS - 1 else 0.0
        y_sum = jnp.where(lane < GZ, below, pltpu.roll(here, GZ, 1)) + jnp.where(
            lane >= LANES - GZ, above, pltpu.roll(here, LANES - GZ, 1))
        lower = jnp.where(along > 0, pltpu.roll(here, 1, 1), 0.0)
        upper = jnp.where(along < GZ - 1, pltpu.roll(here, LANES - 1, 1), 0.0)
        yield j, here, (1.0 - 6.0 * diffusion) * here + diffusion * ((y_sum + lower) + (upper + across(j)))
        before, here = here, after


def kernel(sections, groups, init_ref, ref_hbm, weight_hbm, matrix_hbm, kkt_hbm, bound_ref,
           states_out, boxed_out, dual_out, hist_out,
           ref_ref, weight_ref, kkt_ref, mat, mat_t, S, AS, T, D, dual, wref, recip, lhs, halo,
           send24, send0, own24, low24, high24, own0, low0, high0,
           fold, edge24, part, part_low, part_in, init_in, tile, tile_prev, tile_same, tile_next, k_high, k_low, pul, boxed, scaled,
           hist, first_in, second, second_in,
           load_sem, flat_sem, halo_send, halo_recv, pass_send, pass_recv, init_send, init_recv, send_sem, recv_sem, hist_send, hist_recv):
    s = lax.axis_index("section")
    x = lax.axis_index("state")
    columns = sections // 2

    def inside(ds, dx):
        return (s + ds >= 0) & (s + ds < sections) & (x + dx >= 0) & (x + dx < groups)

    def rotated(d):
        return lax.rem(x + d, groups)

    pair_count = 2 * groups

    def pair_peer(e):
        flat = lax.rem(lax.rem(s, 2) * groups + x + e, pair_count)
        return (s - lax.rem(s, 2) + flat // groups, lax.rem(flat, groups))

    def column_peer(e):
        return (lax.rem(s // 2 + e, columns) * 2 + lax.rem(s, 2), x)

    zeros = lambda ref: ref.__setitem__(Ellipsis, jnp.zeros(ref.shape, ref.dtype))
    for ref in (halo, own24, low24, high24, own0, low0, high0, init_in, edge24):
        zeros(ref)

    barrier = pltpu.get_barrier_semaphore()

    def greet(target):
        pl.semaphore_signal(barrier, inc=1, device_id=target, device_id_type=MESH)

    for d in range(1, groups):
        greet((s, rotated(d)))
    for d in range(groups):
        @pl.when(s > 0)
        def _():
            greet((s - 1, rotated(d)))

        @pl.when(s < sections - 1)
        def _():
            greet((s + 1, rotated(d)))
    for e in range(1, columns):
        greet(column_peer(e))

    loads = [pltpu.make_async_copy(matrix_hbm.at[p], mat.at[p + 1], load_sem.at[p]) for p in range(PLANES)]
    flat_loads = []
    for j in range(CHUNKS):
        cells = pl.ds(j * LANES, LANES)
        flat_loads.append(pltpu.make_async_copy(weight_hbm.at[:, cells], weight_ref.at[j], flat_sem.at[0, j]))
        flat_loads.append(pltpu.make_async_copy(ref_hbm.at[:, cells], ref_ref.at[j], flat_sem.at[1, j]))
    kkt_load = pltpu.make_async_copy(kkt_hbm, kkt_ref, load_sem.at[PLANES])
    for copy in flat_loads + [kkt_load] + loads:
        copy.start()

    for ref in (AS, T, D, dual, S, boxed, scaled, hist):
        zeros(ref)

    @pl.when(x == 0)
    def _():
        mat[0] = jnp.zeros((PLANE, WIDTH), BF16)

    @pl.when(x == groups - 1)
    def _():
        mat[PLANES + 1] = jnp.zeros((PLANE, WIDTH), BF16)

    neighbours = (
        (s > 0).astype(jnp.int32) * groups
        + (s < sections - 1).astype(jnp.int32) * groups
        + (groups - 1)
        + (columns - 1)
    )
    pl.semaphore_wait(barrier, neighbours)

    twin = s + 1 - 2 * lax.rem(s, 2)
    depth = PLANE // BLOCKS

    def mine(block):
        return lax.rem(s, 2) == jnp.where(s < 2, 1, block // (BLOCKS // 2))

    def plane_copy(side, piece):
        source = 0 if side == 0 else PLANES - 1
        target = PLANES + 1 if side == 0 else 0
        rows = pl.ds(piece * depth, depth)
        return pltpu.make_async_remote_copy(
            src_ref=matrix_hbm.at[source, rows], dst_ref=mat.at[target, rows],
            send_sem=halo_send.at[side, piece], recv_sem=halo_recv.at[side, piece],
            device_id=(s, x - 1 if side == 0 else x + 1), device_id_type=MESH)

    def pass_copy(side, piece):
        target = PLANES + 1 if side == 0 else 0
        rows = pl.ds(piece * depth, depth)
        return pltpu.make_async_remote_copy(
            src_ref=mat.at[target, rows], dst_ref=mat.at[target, rows],
            send_sem=pass_send.at[side, piece], recv_sem=pass_recv.at[side, piece],
            device_id=(twin, x), device_id_type=MESH)

    sends_to = (x > 0, x < groups - 1)
    gets_from = (x < groups - 1, x > 0)

    def init_copy(side):
        return pltpu.make_async_remote_copy(
            src_ref=init_ref, dst_ref=init_in.at[1 - side], send_sem=init_send.at[side],
            recv_sem=init_recv.at[side], device_id=(s, x - 1 if side == 0 else x + 1), device_id_type=MESH)

    for side in range(2):
        @pl.when((s == 0) & sends_to[side])
        def _():
            init_copy(side).start()

    for piece in range(BLOCKS):
        for side in range(2):
            @pl.when(sends_to[side] & mine(piece))
            def _():
                plane_copy(side, piece).start()

    kkt_load.wait()
    kkt = kkt_ref[...]
    high = kkt.astype(BF16)
    k_high[...] = high
    k_low[...] = (kkt - high.astype(F32)).astype(BF16)

    for copy in flat_loads:
        copy.wait()
    for p in range(PLANES):
        for j in range(CHUNKS):
            weight = weight_ref[j, pl.ds(p, ROWS, stride=PLANES), :]
            wref[p, j] = weight * ref_ref[j, pl.ds(p, ROWS, stride=PLANES), :]
            recip[p, j] = 1.0 / (weight + 2.0)

    penalty = float(GX * GY * GZ) / WIDTH
    not_last = jnp.where(s < sections - 1, 1.0, 0.0).astype(F32)
    has_side = (jnp.where(x > 0, 1.0, 0.0).astype(F32), jnp.where(x < groups - 1, 1.0, 0.0).astype(F32))
    cross = [(0, -1), (0, 1), (1, 0), (1, 1), (1, -1), (-1, 0), (-1, 1), (-1, -1), (0, -1), (0, 1)]
    base_index = len(cross)

    def messages(slot):
        return [
            (fold.at[0], halo.at[slot, 1]),
            (fold.at[1], halo.at[slot, 0]),
            (send24.at[pl.ds(1, PLANES)], own24.at[slot]),
            (send24.at[PLANES + 1], low24.at[slot]),
            (send24.at[0], high24.at[slot]),
            (send0, own0.at[slot]),
            (send0.at[PLANES - 1], low0.at[slot]),
            (send0.at[0], high0.at[slot]),
            (send24.at[pl.ds(0, 2)], edge24.at[slot, 1]),
            (send24.at[pl.ds(PLANES, 2)], edge24.at[slot, 0]),
        ]

    def cross_copy(i, slot):
        ds, dx = cross[i]
        source, target = messages(slot)[i]
        return pltpu.make_async_remote_copy(
            src_ref=source, dst_ref=target, send_sem=send_sem.at[i], recv_sem=recv_sem.at[slot, i],
            device_id=(s + ds, x + dx), device_id_type=MESH)

    def peer_copy(d, slot):
        i = base_index + d - 1
        return pltpu.make_async_remote_copy(
            src_ref=part_low, dst_ref=part_in.at[slot, d - 1], send_sem=send_sem.at[i],
            recv_sem=recv_sem.at[slot, i], device_id=(s, rotated(d)), device_id_type=MESH)

    def tile_copy(ds, d, slot):
        i = base_index + groups - 1 + groups * (ds + 1) + d
        target = (tile_next, tile_same, tile_prev)[ds + 1]
        return pltpu.make_async_remote_copy(
            src_ref=tile, dst_ref=target.at[slot, d - 1 if ds == 0 else d], send_sem=send_sem.at[i],
            recv_sem=recv_sem.at[slot, i], device_id=(s + ds, rotated(d)), device_id_type=MESH)

    def folded(side, outside, full):
        base = (0 if outside else FOLD) if side == 0 else (FOLD if outside else 0)
        for j in range(CHUNKS):
            fold[side, :, base + j * LANES:base + (j + 1) * LANES] = full[j][0:16].astype(BF16)
        for j in range(CHUNKS // 2):
            pair = jnp.concatenate([full[j][16:24], full[j + CHUNKS // 2][16:24]], 0)
            fold[side, :, base + PLANE + j * LANES:base + PLANE + (j + 1) * LANES] = pair.astype(BF16)

    def unfolded(slot, side, base, j):
        top = halo[slot, side, :, base + j * LANES:base + (j + 1) * LANES].astype(F32)
        i = j % (CHUNKS // 2)
        pair = halo[slot, side, :, base + PLANE + i * LANES:base + PLANE + (i + 1) * LANES].astype(F32)
        start = 8 * (j // (CHUNKS // 2))
        return jnp.concatenate([top, pair[start:start + 8]], 0)

    def apply(p):
        bodies = []
        moved = in_plane(lambda j: S[p + 1, j, 8:32, :], lambda j: S[p, j, 8:32, :] + S[p + 2, j, 8:32, :])
        for j, here, value in moved:
            AS[p, j, 8:32, :] = value
            body = here + dual[p, j] - AS[p, j, pl.ds(7, ROWS), :]
            tail = -AS[p, j, pl.ds(31, 8), :]
            T[p + 1, j, 0:24, :] = body
            T[p + 1, j, 24:32, :] = tail
            lhs[:, (p + 1) * PLANE + j * LANES:(p + 1) * PLANE + (j + 1) * LANES] = jnp.concatenate(
                [body, tail], 0).astype(BF16)
            send24[p + 1, j:j + 1, :] = tail[0:1]
            send0[p, j:j + 1, :] = body[0:1]
            if p in (0, PLANES - 1):
                bodies.append(body)
        if p in (0, PLANES - 1):
            folded(0 if p == 0 else 1, False, bodies)

    def apply_outside(side):
        p, q = ((0, 1), (PLANES + 1, PLANES))[side]
        bodies = []
        for j in range(CHUNKS):
            full = (-diffusion * has_side[side]) * S[q, j, pl.ds(7, 32), :]
            T[p, j] = full
            lhs[:, p * PLANE + j * LANES:p * PLANE + (j + 1) * LANES] = full.astype(BF16)
            send24[p, j:j + 1, :] = full[24:25]
            bodies.append(full)
        folded(side, True, bodies)

    def solve(k, slot):
        total = part[...]
        top, tail, low = total[0:16], total[16:24], total[24:32]
        for d in range(1, groups):
            piece = part_in[slot, d - 1].astype(F32)
            top = top + piece[:, 0:WIDTH]
            tail = tail + jnp.concatenate([piece[0:8, WIDTH:], piece[8:16, WIDTH:]], 1)
        pul[...] = jnp.concatenate([top, tail, low], 0) + penalty * (boxed[...] - scaled[...])

        @pl.when(k > 0)
        def _():
            incoming = tile_same[slot, 0]
            for d in range(2, groups):
                incoming = incoming + tile_same[slot, d - 1]
            for c in range(4):
                cells = slice(c * LANES, (c + 1) * LANES)
                pul[24:25, cells] += incoming[c + 4:c + 5]

        @pl.when((s > 0) & (k > 0))
        def _():
            incoming = tile_prev[slot, 0]
            for d in range(1, groups):
                incoming = incoming + tile_prev[slot, d]
            for c in range(4):
                cells = slice(c * LANES, (c + 1) * LANES)
                pul[0:1, cells] += incoming[c + 4:c + 5]

        @pl.when((s < sections - 1) & (k > 0))
        def _():
            incoming = tile_next[slot, 0]
            for d in range(1, groups):
                incoming = incoming + tile_next[slot, d]
            for c in range(4):
                cells = slice(c * LANES, (c + 1) * LANES)
                pul[24:25, cells] += incoming[c:c + 1]

        rhs = pul[...]
        rhs_high = rhs.astype(BF16)
        rhs_low = (rhs - rhs_high.astype(F32)).astype(BF16)
        stacked = jnp.dot(jnp.concatenate([rhs_high, rhs_low], 0), k_high[...], preferred_element_type=F32)
        inputs = stacked[0:32] + stacked[32:64] + jnp.dot(rhs_high, k_low[...], preferred_element_type=F32)
        bound = bound_ref[...]
        boxed_new = jnp.clip(inputs + scaled[...], -bound, bound)
        gap = inputs - boxed_new
        scaled[...] = scaled[...] + gap
        boxed[...] = boxed_new
        gap_sum = jnp.sum(gap[0:ROWS] * gap[0:ROWS], axis=(0, 1), keepdims=True)
        record(k, 1, gap_sum)
        return inputs.astype(BF16)

    def narrow(value):
        part_low[:, 0:WIDTH] = value[0:16].astype(BF16)
        half = WIDTH // 2
        part_low[:, WIDTH:] = jnp.concatenate([value[16:24, 0:half], value[16:24, half:]], 0).astype(BF16)

    def record(k, kind, value):
        row = lax.broadcasted_iota(jnp.int32, (8, LANES), 0)
        column = lax.broadcasted_iota(jnp.int32, (8, LANES), 1)
        hist[...] += jnp.where((row == kind) & (column == k), value, 0.0)

    def drive(p, inputs_low):
        for i in range(PLANE // 256):
            driven = jnp.dot(inputs_low, mat_t[p, :, i * 256:(i + 1) * 256], preferred_element_type=F32)
            for j in (2 * i, 2 * i + 1):
                piece = driven[:, (j % 2) * LANES:(j % 2 + 1) * LANES]
                D[p, j, 0:24, :] = T[p, j, 0:24, :] - piece[0:24]
                D[p, j, 24:32, :] = (T[p, j, 24:32, :] - piece[24:32]) * not_last

    def update(p, acc):
        back = in_plane(lambda j: D[p + 1, j, pl.ds(1, ROWS), :],
                        lambda j: D[p, j, pl.ds(1, ROWS), :] + D[p + 2, j, pl.ds(1, ROWS), :])
        for j, _, value in back:
            old = S[p + 1, j, 8:32, :]
            defect = D[p + 1, j, 0:24, :]
            fresh = (wref[p, j] + (2.0 * old - defect) + value) * recip[p, j]
            old_dual = dual[p, j]
            new_dual = fresh - old + defect
            primal = new_dual - old_dual
            S[p + 1, j, 8:32, :] = fresh
            dual[p, j] = new_dual
            square = primal * primal
            acc = acc + (square[0:8] + square[8:16] + square[16:24])
        return acc

    def record_primal(k, acc):
        record(k, 0, jnp.sum(acc, axis=(0, 1), keepdims=True))

    for copy in loads:
        copy.wait()

    @pl.when(s == 0)
    def _():
        for side in range(2):
            @pl.when(gets_from[side])
            def _():
                init_copy(side).wait_recv()

            @pl.when(sends_to[side])
            def _():
                init_copy(side).wait_send()
        for p in range(PLANES):
            def own(j):
                return init_ref[p:p + 1, j * LANES:(j + 1) * LANES]

            def beside(j):
                cells = slice(j * LANES, (j + 1) * LANES)
                below = init_ref[p - 1:p, cells] if p > 0 else init_in[0, PLANES - 1:PLANES, cells]
                above = init_ref[p + 1:p + 2, cells] if p < PLANES - 1 else init_in[1, 0:1, cells]
                return below + above

            for j, _, value in in_plane(own, beside):
                AS[p, j, 7:8, :] = value
        for p in range(PLANES):
            apply(p)
        part[...] = jnp.dot(lhs[:, PLANE:(PLANES + 1) * PLANE],
                            mat[1:PLANES + 1].reshape(PLANES * PLANE, WIDTH), preferred_element_type=F32)
        narrow(part[...])
        for d in range(1, groups):
            peer_copy(d, 0).start()

    def turn(p, carry):
        mat_t[p] = mat[p].T
        return carry

    lax.fori_loop(1, PLANES + 1, turn, 0)

    @pl.when(s == 0)
    def _():
        for d in range(1, groups):
            peer_copy(d, 0).wait_recv()
        inputs_low = solve(0, 0)
        for p in range(PLANES):
            drive(p + 1, inputs_low)
        for d in range(1, groups):
            peer_copy(d, 0).wait_send()

    acc = jnp.zeros((8, LANES), F32)
    for p in range(PLANES):
        acc = update(p, acc)
    record_primal(0, acc)
    for p in range(PLANES):
        apply(p)
    apply_outside(0)
    apply_outside(1)

    for piece in range(BLOCKS):
        for side in range(2):
            @pl.when(gets_from[side] & mine(piece))
            def _():
                plane_copy(side, piece).wait_recv()
                pass_copy(side, piece).start()
    for piece in range(BLOCKS):
        for side in range(2):
            @pl.when(gets_from[side] & jnp.logical_not(mine(piece)))
            def _():
                pass_copy(side, piece).wait_recv()

            @pl.when(gets_from[side] & mine(piece))
            def _():
                pass_copy(side, piece).wait_send()

            @pl.when(sends_to[side] & mine(piece))
            def _():
                plane_copy(side, piece).wait_send()
    mat_t[0] = mat[0].T
    mat_t[PLANES + 1] = mat[PLANES + 1].T

    early = 1

    def start_cross(i, slot):
        ds, dx = cross[i]

        @pl.when(inside(ds, dx))
        def _():
            cross_copy(i, slot).start()

    start_cross(early, 1)

    def iteration(k, carry):
        slot = lax.rem(k, 2)
        for i in range(len(cross)):
            if i != early:
                start_cross(i, slot)

        pulled = jnp.dot(lhs[...], mat[...].reshape((PLANES + 2) * PLANE, WIDTH), preferred_element_type=F32)
        narrow(pulled)
        for c in range(4):
            cells = slice(c * LANES, (c + 1) * LANES)
            tile[c:c + 1, :] = pulled[0:1, cells]
            tile[c + 4:c + 5, :] = pulled[24:25, cells]
        part[...] = pulled
        for d in range(groups):
            @pl.when(s < sections - 1)
            def _():
                tile_copy(1, d, slot).start()

            @pl.when(s > 0)
            def _():
                tile_copy(-1, d, slot).start()
        for d in (2, 1, 3):
            peer_copy(d, slot).start()
            tile_copy(0, d, slot).start()

        for i, (ds, dx) in enumerate(cross):
            @pl.when(inside(-ds, -dx))
            def _():
                cross_copy(i, slot).wait_recv()

        for j in range(CHUNKS):
            T[0, j, 0:24, :] += unfolded(slot, 0, 0, j)
            T[1, j, 0:24, :] += unfolded(slot, 0, FOLD, j)
            T[PLANES, j, 0:24, :] += unfolded(slot, 1, 0, j)
            T[PLANES + 1, j, 0:24, :] += unfolded(slot, 1, FOLD, j)
            T[0, j, 24:25, :] += low0[slot, j:j + 1, :] + edge24[slot, 0, 0, j:j + 1, :]
            T[1, j, 24:25, :] += edge24[slot, 0, 1, j:j + 1, :]
            T[PLANES, j, 24:25, :] += edge24[slot, 1, 0, j:j + 1, :]
            T[PLANES + 1, j, 24:25, :] += high0[slot, j:j + 1, :] + edge24[slot, 1, 1, j:j + 1, :]
            T[1, j, 0:1, :] += low24[slot, j:j + 1, :]
            T[PLANES, j, 0:1, :] += high24[slot, j:j + 1, :]
        for p in range(PLANES):
            for j in range(CHUNKS):
                T[p + 1, j, 0:1, :] += own24[slot, p, j:j + 1, :]
                T[p + 1, j, 24:25, :] += own0[slot, p, j:j + 1, :]

        for i, (ds, dx) in enumerate(cross):
            @pl.when(inside(ds, dx))
            def _():
                cross_copy(i, slot).wait_send()

        for d in range(1, groups):
            peer_copy(d, slot).wait_recv()
            tile_copy(0, d, slot).wait_recv()
        for d in range(groups):
            @pl.when(s > 0)
            def _():
                tile_copy(1, d, slot).wait_recv()

            @pl.when(s < sections - 1)
            def _():
                tile_copy(-1, d, slot).wait_recv()
        inputs_low = solve(k, slot)

        acc = jnp.zeros((8, LANES), F32)
        for q in range(PLANES + 1, -1, -1):
            drive(q, inputs_low)
            if q < PLANES:
                acc = update(q, acc)
            if q < PLANES - 1:
                apply(q + 1)
            if q == PLANES - 2:
                apply_outside(1)

                @pl.when(k < ITERS - 1)
                def _():
                    start_cross(early, 1 - slot)
        apply(0)
        apply_outside(0)
        record_primal(k, acc)

        for d in range(1, groups):
            peer_copy(d, slot).wait_send()
            tile_copy(0, d, slot).wait_send()
        for d in range(groups):
            @pl.when(s < sections - 1)
            def _():
                tile_copy(1, d, slot).wait_send()

            @pl.when(s > 0)
            def _():
                tile_copy(-1, d, slot).wait_send()
        return carry

    lax.fori_loop(1, ITERS, iteration, 0)

    def first_copy(e):
        return pltpu.make_async_remote_copy(
            src_ref=hist, dst_ref=first_in.at[e - 1], send_sem=hist_send.at[e - 1], recv_sem=hist_recv.at[e - 1],
            device_id=pair_peer(e), device_id_type=MESH)

    def second_copy(e):
        i = pair_count - 2 + e
        return pltpu.make_async_remote_copy(
            src_ref=second, dst_ref=second_in.at[e - 1], send_sem=hist_send.at[i], recv_sem=hist_recv.at[i],
            device_id=column_peer(e), device_id_type=MESH)

    for e in range(1, pair_count):
        first_copy(e).start()

    for p in range(PLANES):
        for j in range(CHUNKS):
            ref_ref[j, pl.ds(p, ROWS, stride=PLANES), :] = S[p + 1, j, 8:32, :]
            weight_ref[j, pl.ds(p, ROWS, stride=PLANES), :] = dual[p, j]
    stores = [
        pltpu.make_async_copy(ref_ref, states_out, flat_sem.at[0, 0]),
        pltpu.make_async_copy(weight_ref, dual_out, flat_sem.at[1, 0]),
    ]
    for copy in stores:
        copy.start()
    boxed_out[...] = boxed[0:ROWS]

    for e in range(1, pair_count):
        first_copy(e).wait()
    total = hist[...]
    for e in range(1, pair_count):
        total = total + first_in[e - 1]
    second[...] = total
    for e in range(1, columns):
        second_copy(e).start()
    for e in range(1, columns):
        second_copy(e).wait()
    for e in range(1, columns):
        total = total + second_in[e - 1]
    row = lax.broadcasted_iota(jnp.int32, (8, LANES), 0)
    cells = float(ROWS * sections * GX * GY * GZ)
    inputs_count = float(ROWS * sections * WIDTH * groups)
    for copy in stores:
        copy.wait()
    hist_out[...] = jnp.sqrt(jnp.where(row == 0, total * (1.0 / cells), total * (1.0 / inputs_count)) + epsilon)


def deliver(states, boxed, dual_vars, record, states_out, boxed_out, dual_out, record_out, a, b, sem):
    loads, stores = [], []
    for i, (source, held, target) in enumerate(((states, a, states_out), (dual_vars, b, dual_out))):
        for j in range(CHUNKS):
            cells = pl.ds(j * LANES, LANES)
            loads.append(pltpu.make_async_copy(source.at[j], held.at[j], sem.at[i, j]))
            stores.append(pltpu.make_async_copy(held.at[j], target.at[:, cells], sem.at[2 + i, j]))
    for copy in loads:
        copy.start()
    boxed_out[...] = boxed[...]
    record_out[...] = record[0:2, 0:ITERS]
    for load, store in zip(loads, stores):
        load.wait()
        store.start()
    for copy in stores:
        copy.wait()


def solution(mesh):
    sections, groups = mesh.shape["section"], mesh.shape["state"]
    columns = sections // 2

    def local(initial_state, state_ref, state_weight, input_matrix, kkt_inverse, input_bound):
        vmem = pl.BlockSpec(memory_space=pltpu.VMEM)
        any_space = pl.BlockSpec(memory_space=pl.ANY)
        flat = (ROWS * PLANES, PLANE)
        chunked = (CHUNKS, ROWS * PLANES, LANES)
        V = pltpu.VMEM
        DMA = pltpu.SemaphoreType.DMA
        message_count = 10 + groups - 1 + 3 * groups
        compact = (CHUNKS, LANES)
        states, boxed, dual_vars, record = pl.pallas_call(
            functools.partial(kernel, sections, groups),
            out_shape=(
                jax.ShapeDtypeStruct(chunked, F32),
                jax.ShapeDtypeStruct((ROWS, WIDTH), F32),
                jax.ShapeDtypeStruct(chunked, F32),
                jax.ShapeDtypeStruct((8, LANES), F32),
            ),
            in_specs=[vmem, any_space, any_space, any_space, any_space, vmem],
            out_specs=(any_space, vmem, any_space, vmem),
            scratch_shapes=[
                V((CHUNKS, ROWS * PLANES, LANES), F32),
                V((CHUNKS, ROWS * PLANES, LANES), F32),
                V((WIDTH, WIDTH), F32),
                V((PLANES + 2, PLANE, WIDTH), BF16),
                V((PLANES + 2, WIDTH, PLANE), BF16),
                V((PLANES + 2, CHUNKS, 40, LANES), F32),
                V((PLANES, CHUNKS, 40, LANES), F32),
                V((PLANES + 2, CHUNKS, 32, LANES), F32),
                V((PLANES + 2, CHUNKS, 32, LANES), F32),
                V((PLANES, CHUNKS, ROWS, LANES), F32),
                V((PLANES, CHUNKS, ROWS, LANES), F32),
                V((PLANES, CHUNKS, ROWS, LANES), F32),
                V((32, (PLANES + 2) * PLANE), BF16),
                V((2, 2, 16, 2 * FOLD), BF16),
                V((PLANES + 2, *compact), F32),
                V((PLANES, *compact), F32),
                V((2, PLANES, *compact), F32),
                V((2, *compact), F32),
                V((2, *compact), F32),
                V((2, PLANES, *compact), F32),
                V((2, *compact), F32),
                V((2, *compact), F32),
                V((2, 16, 2 * FOLD), BF16),
                V((2, 2, 2, *compact), F32),
                V((32, WIDTH), F32),
                V((16, WIDTH + WIDTH // 2), BF16),
                V((2, groups - 1, 16, WIDTH + WIDTH // 2), BF16),
                V((2, PLANES, PLANE), F32),
                V(compact, F32),
                V((2, groups, *compact), F32),
                V((2, groups - 1, *compact), F32),
                V((2, groups, *compact), F32),
                V((WIDTH, WIDTH), BF16),
                V((WIDTH, WIDTH), BF16),
                V((32, WIDTH), F32),
                V((32, WIDTH), F32),
                V((32, WIDTH), F32),
                V(compact, F32),
                V((2 * groups - 1, *compact), F32),
                V(compact, F32),
                V((max(columns - 1, 1), *compact), F32),
                DMA((PLANES + 1,)),
                DMA((2, CHUNKS)),
                DMA((2, BLOCKS)),
                DMA((2, BLOCKS)),
                DMA((2, BLOCKS)),
                DMA((2, BLOCKS)),
                DMA((2,)),
                DMA((2,)),
                DMA((message_count,)),
                DMA((2, message_count)),
                DMA((2 * groups + columns,)),
                DMA((2 * groups + columns,)),
            ],
            compiler_params=pltpu.CompilerParams(
                collective_id=0, has_side_effects=True, vmem_limit_bytes=64000 * 1024),
        )(
            initial_state,
            state_ref.reshape(flat),
            state_weight.reshape(flat),
            input_matrix,
            kkt_inverse,
            input_bound.reshape(1, WIDTH),
        )
        states, boxed, dual_vars, record = pl.pallas_call(
            deliver,
            out_shape=(
                jax.ShapeDtypeStruct(flat, F32),
                jax.ShapeDtypeStruct((ROWS, WIDTH), F32),
                jax.ShapeDtypeStruct(flat, F32),
                jax.ShapeDtypeStruct((2, ITERS), F32),
            ),
            in_specs=[any_space, vmem, any_space, vmem],
            out_specs=(any_space, vmem, any_space, vmem),
            scratch_shapes=[V(chunked, F32), V(chunked, F32), DMA((4, CHUNKS))],
        )(states, boxed, dual_vars, record)
        return (states.reshape(state_ref.shape), boxed, dual_vars.reshape(state_ref.shape), record.T)

    return jax.shard_map(
        local,
        mesh=mesh,
        in_specs=(
            P("state", None),
            P("section", "state", None),
            P("section", "state", None),
            P("state", None, None),
            P(),
            P(),
        ),
        out_specs=(P("section", "state", None), P("section", None), P("section", "state", None), P()),
        check_vma=False,
    )
```

```python
import functools

import jax
import jax.numpy as jnp
from jax import lax
from jax.experimental import pallas as pl
from jax.experimental.pallas import tpu as pltpu
from jax.sharding import PartitionSpec as P

GX = 32
GY = 32
GZ = 32
ITERS = 10
BLOCKS = 8
FOLD = 1536
PLANES = 8
CHUNKS = 8
ROWS = 24
LANES = 128
WIDTH = 512
PLANE = 1024
diffusion = 0.15
epsilon = 1e-06
MESH = pl.DeviceIdType.MESH
F32 = jnp.float32
BF16 = jnp.bfloat16


def in_plane(chunk, across):
    lane = lax.broadcasted_iota(jnp.int32, (1, LANES), 1)
    along = lane % GZ
    here = chunk(0)
    before = None
    for j in range(CHUNKS):
        after = chunk(j + 1) if j < CHUNKS - 1 else None
        below = pltpu.roll(before, GZ, 1) if j > 0 else 0.0
        above = pltpu.roll(after, LANES - GZ, 1) if j < CHUNKS - 1 else 0.0
        y_sum = jnp.where(lane < GZ, below, pltpu.roll(here, GZ, 1)) + jnp.where(
            lane >= LANES - GZ, above, pltpu.roll(here, LANES - GZ, 1))
        lower = jnp.where(along > 0, pltpu.roll(here, 1, 1), 0.0)
        upper = jnp.where(along < GZ - 1, pltpu.roll(here, LANES - 1, 1), 0.0)
        yield j, here, (1.0 - 6.0 * diffusion) * here + diffusion * ((y_sum + lower) + (upper + across(j)))
        before, here = here, after


def kernel(sections, groups, init_ref, ref_hbm, weight_hbm, matrix_hbm, kkt_hbm, bound_ref,
           states_out, boxed_out, dual_out, hist_out,
           ref_ref, weight_ref, kkt_ref, mat, mat_t, S, AS, T, D, dual, wref, recip, lhs, halo,
           send24, send0, own24, low24, high24, own0, low0, high0,
           fold, edge24, part, part_low, part_in, init_in, tile, tile_prev, tile_same, tile_next, k_high, k_low, pul, boxed, scaled,
           hist, first_in, second, second_in,
           load_sem, flat_sem, halo_send, halo_recv, pass_send, pass_recv, init_send, init_recv, send_sem, recv_sem, hist_send, hist_recv):
    s = lax.axis_index("section")
    x = lax.axis_index("state")
    columns = sections // 2

    def inside(ds, dx):
        return (s + ds >= 0) & (s + ds < sections) & (x + dx >= 0) & (x + dx < groups)

    def rotated(d):
        return lax.rem(x + d, groups)

    pair_count = 2 * groups

    def pair_peer(e):
        flat = lax.rem(lax.rem(s, 2) * groups + x + e, pair_count)
        return (s - lax.rem(s, 2) + flat // groups, lax.rem(flat, groups))

    def column_peer(e):
        return (lax.rem(s // 2 + e, columns) * 2 + lax.rem(s, 2), x)

    zeros = lambda ref: ref.__setitem__(Ellipsis, jnp.zeros(ref.shape, ref.dtype))
    for ref in (halo, own24, low24, high24, own0, low0, high0, init_in, edge24):
        zeros(ref)

    barrier = pltpu.get_barrier_semaphore()

    def greet(target):
        pl.semaphore_signal(barrier, inc=1, device_id=target, device_id_type=MESH)

    for d in range(1, groups):
        greet((s, rotated(d)))
    for d in range(groups):
        @pl.when(s > 0)
        def _():
            greet((s - 1, rotated(d)))

        @pl.when(s < sections - 1)
        def _():
            greet((s + 1, rotated(d)))
    for e in range(1, columns):
        greet(column_peer(e))

    loads = [pltpu.make_async_copy(matrix_hbm.at[p], mat.at[p + 1], load_sem.at[p]) for p in range(PLANES)]
    flat_loads = []
    for j in range(CHUNKS):
        cells = pl.ds(j * LANES, LANES)
        flat_loads.append(pltpu.make_async_copy(weight_hbm.at[:, cells], weight_ref.at[j], flat_sem.at[0, j]))
        flat_loads.append(pltpu.make_async_copy(ref_hbm.at[:, cells], ref_ref.at[j], flat_sem.at[1, j]))
    kkt_load = pltpu.make_async_copy(kkt_hbm, kkt_ref, load_sem.at[PLANES])
    for copy in flat_loads + [kkt_load] + loads:
        copy.start()

    for ref in (AS, T, D, dual, S, boxed, scaled, hist):
        zeros(ref)

    @pl.when(x == 0)
    def _():
        mat[0] = jnp.zeros((PLANE, WIDTH), BF16)

    @pl.when(x == groups - 1)
    def _():
        mat[PLANES + 1] = jnp.zeros((PLANE, WIDTH), BF16)

    neighbours = (
        (s > 0).astype(jnp.int32) * groups
        + (s < sections - 1).astype(jnp.int32) * groups
        + (groups - 1)
        + (columns - 1)
    )
    pl.semaphore_wait(barrier, neighbours)

    twin = s + 1 - 2 * lax.rem(s, 2)
    depth = PLANE // BLOCKS

    def mine(block):
        return lax.rem(s, 2) == jnp.where(s < 2, 1, block // (BLOCKS // 2))

    def plane_copy(side, piece):
        source = 0 if side == 0 else PLANES - 1
        target = PLANES + 1 if side == 0 else 0
        rows = pl.ds(piece * depth, depth)
        return pltpu.make_async_remote_copy(
            src_ref=matrix_hbm.at[source, rows], dst_ref=mat.at[target, rows],
            send_sem=halo_send.at[side, piece], recv_sem=halo_recv.at[side, piece],
            device_id=(s, x - 1 if side == 0 else x + 1), device_id_type=MESH)

    def pass_copy(side, piece):
        target = PLANES + 1 if side == 0 else 0
        rows = pl.ds(piece * depth, depth)
        return pltpu.make_async_remote_copy(
            src_ref=mat.at[target, rows], dst_ref=mat.at[target, rows],
            send_sem=pass_send.at[side, piece], recv_sem=pass_recv.at[side, piece],
            device_id=(twin, x), device_id_type=MESH)

    sends_to = (x > 0, x < groups - 1)
    gets_from = (x < groups - 1, x > 0)

    def init_copy(side):
        return pltpu.make_async_remote_copy(
            src_ref=init_ref, dst_ref=init_in.at[1 - side], send_sem=init_send.at[side],
            recv_sem=init_recv.at[side], device_id=(s, x - 1 if side == 0 else x + 1), device_id_type=MESH)

    for side in range(2):
        @pl.when((s == 0) & sends_to[side])
        def _():
            init_copy(side).start()

    for piece in range(BLOCKS):
        for side in range(2):
            @pl.when(sends_to[side] & mine(piece))
            def _():
                plane_copy(side, piece).start()

    kkt_load.wait()
    kkt = kkt_ref[...]
    high = kkt.astype(BF16)
    k_high[...] = high
    k_low[...] = (kkt - high.astype(F32)).astype(BF16)

    for copy in flat_loads:
        copy.wait()
    for p in range(PLANES):
        for j in range(CHUNKS):
            weight = weight_ref[j, pl.ds(p, ROWS, stride=PLANES), :]
            wref[p, j] = weight * ref_ref[j, pl.ds(p, ROWS, stride=PLANES), :]
            recip[p, j] = 1.0 / (weight + 2.0)

    penalty = float(GX * GY * GZ) / WIDTH
    not_last = jnp.where(s < sections - 1, 1.0, 0.0).astype(F32)
    has_side = (jnp.where(x > 0, 1.0, 0.0).astype(F32), jnp.where(x < groups - 1, 1.0, 0.0).astype(F32))
    cross = [(0, -1), (0, 1), (1, 0), (1, 1), (1, -1), (-1, 0), (-1, 1), (-1, -1), (0, -1), (0, 1)]
    base_index = len(cross)

    def messages(slot):
        return [
            (fold.at[0], halo.at[slot, 1]),
            (fold.at[1], halo.at[slot, 0]),
            (send24.at[pl.ds(1, PLANES)], own24.at[slot]),
            (send24.at[PLANES + 1], low24.at[slot]),
            (send24.at[0], high24.at[slot]),
            (send0, own0.at[slot]),
            (send0.at[PLANES - 1], low0.at[slot]),
            (send0.at[0], high0.at[slot]),
            (send24.at[pl.ds(0, 2)], edge24.at[slot, 1]),
            (send24.at[pl.ds(PLANES, 2)], edge24.at[slot, 0]),
        ]

    def cross_copy(i, slot):
        ds, dx = cross[i]
        source, target = messages(slot)[i]
        return pltpu.make_async_remote_copy(
            src_ref=source, dst_ref=target, send_sem=send_sem.at[i], recv_sem=recv_sem.at[slot, i],
            device_id=(s + ds, x + dx), device_id_type=MESH)

    def peer_copy(d, slot):
        i = base_index + d - 1
        return pltpu.make_async_remote_copy(
            src_ref=part_low, dst_ref=part_in.at[slot, d - 1], send_sem=send_sem.at[i],
            recv_sem=recv_sem.at[slot, i], device_id=(s, rotated(d)), device_id_type=MESH)

    def tile_copy(ds, d, slot):
        i = base_index + groups - 1 + groups * (ds + 1) + d
        target = (tile_next, tile_same, tile_prev)[ds + 1]
        return pltpu.make_async_remote_copy(
            src_ref=tile, dst_ref=target.at[slot, d - 1 if ds == 0 else d], send_sem=send_sem.at[i],
            recv_sem=recv_sem.at[slot, i], device_id=(s + ds, rotated(d)), device_id_type=MESH)

    def folded(side, outside, full):
        base = (0 if outside else FOLD) if side == 0 else (FOLD if outside else 0)
        for j in range(CHUNKS):
            fold[side, :, base + j * LANES:base + (j + 1) * LANES] = full[j][0:16].astype(BF16)
        for j in range(CHUNKS // 2):
            pair = jnp.concatenate([full[j][16:24], full[j + CHUNKS // 2][16:24]], 0)
            fold[side, :, base + PLANE + j * LANES:base + PLANE + (j + 1) * LANES] = pair.astype(BF16)

    def unfolded(slot, side, base, j):
        top = halo[slot, side, :, base + j * LANES:base + (j + 1) * LANES].astype(F32)
        i = j % (CHUNKS // 2)
        pair = halo[slot, side, :, base + PLANE + i * LANES:base + PLANE + (i + 1) * LANES].astype(F32)
        start = 8 * (j // (CHUNKS // 2))
        return jnp.concatenate([top, pair[start:start + 8]], 0)

    def apply(p):
        bodies = []
        moved = in_plane(lambda j: S[p + 1, j, 8:32, :], lambda j: S[p, j, 8:32, :] + S[p + 2, j, 8:32, :])
        for j, here, value in moved:
            AS[p, j, 8:32, :] = value
            body = here + dual[p, j] - AS[p, j, pl.ds(7, ROWS), :]
            tail = -AS[p, j, pl.ds(31, 8), :]
            T[p + 1, j, 0:24, :] = body
            T[p + 1, j, 24:32, :] = tail
            lhs[:, (p + 1) * PLANE + j * LANES:(p + 1) * PLANE + (j + 1) * LANES] = jnp.concatenate(
                [body, tail], 0).astype(BF16)
            send24[p + 1, j:j + 1, :] = tail[0:1]
            send0[p, j:j + 1, :] = body[0:1]
            if p in (0, PLANES - 1):
                bodies.append(body)
        if p in (0, PLANES - 1):
            folded(0 if p == 0 else 1, False, bodies)

    def apply_outside(side):
        p, q = ((0, 1), (PLANES + 1, PLANES))[side]
        bodies = []
        for j in range(CHUNKS):
            full = (-diffusion * has_side[side]) * S[q, j, pl.ds(7, 32), :]
            T[p, j] = full
            lhs[:, p * PLANE + j * LANES:p * PLANE + (j + 1) * LANES] = full.astype(BF16)
            send24[p, j:j + 1, :] = full[24:25]
            bodies.append(full)
        folded(side, True, bodies)

    def solve(k, slot):
        total = part[...]
        top, tail, low = total[0:16], total[16:24], total[24:32]
        for d in range(1, groups):
            piece = part_in[slot, d - 1].astype(F32)
            top = top + piece[:, 0:WIDTH]
            tail = tail + jnp.concatenate([piece[0:8, WIDTH:], piece[8:16, WIDTH:]], 1)
        pul[...] = jnp.concatenate([top, tail, low], 0) + penalty * (boxed[...] - scaled[...])

        @pl.when(k > 0)
        def _():
            incoming = tile_same[slot, 0]
            for d in range(2, groups):
                incoming = incoming + tile_same[slot, d - 1]
            for c in range(4):
                cells = slice(c * LANES, (c + 1) * LANES)
                pul[24:25, cells] += incoming[c + 4:c + 5]

        @pl.when((s > 0) & (k > 0))
        def _():
            incoming = tile_prev[slot, 0]
            for d in range(1, groups):
                incoming = incoming + tile_prev[slot, d]
            for c in range(4):
                cells = slice(c * LANES, (c + 1) * LANES)
                pul[0:1, cells] += incoming[c + 4:c + 5]

        @pl.when((s < sections - 1) & (k > 0))
        def _():
            incoming = tile_next[slot, 0]
            for d in range(1, groups):
                incoming = incoming + tile_next[slot, d]
            for c in range(4):
                cells = slice(c * LANES, (c + 1) * LANES)
                pul[24:25, cells] += incoming[c:c + 1]

        rhs = pul[...]
        rhs_high = rhs.astype(BF16)
        rhs_low = (rhs - rhs_high.astype(F32)).astype(BF16)
        stacked = jnp.dot(jnp.concatenate([rhs_high, rhs_low], 0), k_high[...], preferred_element_type=F32)
        inputs = stacked[0:32] + stacked[32:64] + jnp.dot(rhs_high, k_low[...], preferred_element_type=F32)
        bound = bound_ref[...]
        boxed_new = jnp.clip(inputs + scaled[...], -bound, bound)
        gap = inputs - boxed_new
        scaled[...] = scaled[...] + gap
        boxed[...] = boxed_new
        gap_sum = jnp.sum(gap[0:ROWS] * gap[0:ROWS], axis=(0, 1), keepdims=True)
        record(k, 1, gap_sum)
        return inputs.astype(BF16)

    def narrow(value):
        part_low[:, 0:WIDTH] = value[0:16].astype(BF16)
        half = WIDTH // 2
        part_low[:, WIDTH:] = jnp.concatenate([value[16:24, 0:half], value[16:24, half:]], 0).astype(BF16)

    def record(k, kind, value):
        row = lax.broadcasted_iota(jnp.int32, (8, LANES), 0)
        column = lax.broadcasted_iota(jnp.int32, (8, LANES), 1)
        hist[...] += jnp.where((row == kind) & (column == k), value, 0.0)

    def drive(p, inputs_low):
        for i in range(PLANE // 256):
            driven = jnp.dot(inputs_low, mat_t[p, :, i * 256:(i + 1) * 256], preferred_element_type=F32)
            for j in (2 * i, 2 * i + 1):
                piece = driven[:, (j % 2) * LANES:(j % 2 + 1) * LANES]
                D[p, j, 0:24, :] = T[p, j, 0:24, :] - piece[0:24]
                D[p, j, 24:32, :] = (T[p, j, 24:32, :] - piece[24:32]) * not_last

    def update(p, acc):
        back = in_plane(lambda j: D[p + 1, j, pl.ds(1, ROWS), :],
                        lambda j: D[p, j, pl.ds(1, ROWS), :] + D[p + 2, j, pl.ds(1, ROWS), :])
        for j, _, value in back:
            old = S[p + 1, j, 8:32, :]
            defect = D[p + 1, j, 0:24, :]
            fresh = (wref[p, j] + (2.0 * old - defect) + value) * recip[p, j]
            old_dual = dual[p, j]
            new_dual = fresh - old + defect
            primal = new_dual - old_dual
            S[p + 1, j, 8:32, :] = fresh
            dual[p, j] = new_dual
            square = primal * primal
            acc = acc + (square[0:8] + square[8:16] + square[16:24])
        return acc

    def record_primal(k, acc):
        record(k, 0, jnp.sum(acc, axis=(0, 1), keepdims=True))

    for copy in loads:
        copy.wait()

    @pl.when(s == 0)
    def _():
        for side in range(2):
            @pl.when(gets_from[side])
            def _():
                init_copy(side).wait_recv()

            @pl.when(sends_to[side])
            def _():
                init_copy(side).wait_send()
        for p in range(PLANES):
            def own(j):
                return init_ref[p:p + 1, j * LANES:(j + 1) * LANES]

            def beside(j):
                cells = slice(j * LANES, (j + 1) * LANES)
                below = init_ref[p - 1:p, cells] if p > 0 else init_in[0, PLANES - 1:PLANES, cells]
                above = init_ref[p + 1:p + 2, cells] if p < PLANES - 1 else init_in[1, 0:1, cells]
                return below + above

            for j, _, value in in_plane(own, beside):
                AS[p, j, 7:8, :] = value
        for p in range(PLANES):
            apply(p)
        part[...] = jnp.dot(lhs[:, PLANE:(PLANES + 1) * PLANE],
                            mat[1:PLANES + 1].reshape(PLANES * PLANE, WIDTH), preferred_element_type=F32)
        narrow(part[...])
        for d in range(1, groups):
            peer_copy(d, 0).start()

    def turn(p, carry):
        mat_t[p] = mat[p].T
        return carry

    lax.fori_loop(1, PLANES + 1, turn, 0)

    @pl.when(s == 0)
    def _():
        for d in range(1, groups):
            peer_copy(d, 0).wait_recv()
        inputs_low = solve(0, 0)
        for p in range(PLANES):
            drive(p + 1, inputs_low)
        for d in range(1, groups):
            peer_copy(d, 0).wait_send()

    acc = jnp.zeros((8, LANES), F32)
    for p in range(PLANES):
        acc = update(p, acc)
    record_primal(0, acc)
    for p in range(PLANES):
        apply(p)
    apply_outside(0)
    apply_outside(1)

    for piece in range(BLOCKS):
        for side in range(2):
            @pl.when(gets_from[side] & mine(piece))
            def _():
                plane_copy(side, piece).wait_recv()
                pass_copy(side, piece).start()
    for piece in range(BLOCKS):
        for side in range(2):
            @pl.when(gets_from[side] & jnp.logical_not(mine(piece)))
            def _():
                pass_copy(side, piece).wait_recv()

            @pl.when(gets_from[side] & mine(piece))
            def _():
                pass_copy(side, piece).wait_send()

            @pl.when(sends_to[side] & mine(piece))
            def _():
                plane_copy(side, piece).wait_send()

    early = 1

    def start_cross(i, slot):
        ds, dx = cross[i]

        @pl.when(inside(ds, dx))
        def _():
            cross_copy(i, slot).start()

    start_cross(early, 1)

    def iteration(k, carry):
        slot = lax.rem(k, 2)
        for i in range(len(cross)):
            if i != early:
                start_cross(i, slot)

        pulled = jnp.dot(lhs[...], mat[...].reshape((PLANES + 2) * PLANE, WIDTH), preferred_element_type=F32)
        narrow(pulled)
        for c in range(4):
            cells = slice(c * LANES, (c + 1) * LANES)
            tile[c:c + 1, :] = pulled[0:1, cells]
            tile[c + 4:c + 5, :] = pulled[24:25, cells]
        part[...] = pulled
        for d in range(groups):
            @pl.when(s < sections - 1)
            def _():
                tile_copy(1, d, slot).start()

            @pl.when(s > 0)
            def _():
                tile_copy(-1, d, slot).start()
        for d in (2, 1, 3):
            peer_copy(d, slot).start()
            tile_copy(0, d, slot).start()

        @pl.when(k == 1)
        def _():
            mat_t[0] = mat[0].T
            mat_t[PLANES + 1] = mat[PLANES + 1].T

        for i, (ds, dx) in enumerate(cross):
            @pl.when(inside(-ds, -dx))
            def _():
                cross_copy(i, slot).wait_recv()

        for j in range(CHUNKS):
            T[0, j, 0:24, :] += unfolded(slot, 0, 0, j)
            T[1, j, 0:24, :] += unfolded(slot, 0, FOLD, j)
            T[PLANES, j, 0:24, :] += unfolded(slot, 1, 0, j)
            T[PLANES + 1, j, 0:24, :] += unfolded(slot, 1, FOLD, j)
            T[0, j, 24:25, :] += low0[slot, j:j + 1, :] + edge24[slot, 0, 0, j:j + 1, :]
            T[1, j, 24:25, :] += edge24[slot, 0, 1, j:j + 1, :]
            T[PLANES, j, 24:25, :] += edge24[slot, 1, 0, j:j + 1, :]
            T[PLANES + 1, j, 24:25, :] += high0[slot, j:j + 1, :] + edge24[slot, 1, 1, j:j + 1, :]
            T[1, j, 0:1, :] += low24[slot, j:j + 1, :]
            T[PLANES, j, 0:1, :] += high24[slot, j:j + 1, :]
        for p in range(PLANES):
            for j in range(CHUNKS):
                T[p + 1, j, 0:1, :] += own24[slot, p, j:j + 1, :]
                T[p + 1, j, 24:25, :] += own0[slot, p, j:j + 1, :]

        for i, (ds, dx) in enumerate(cross):
            @pl.when(inside(ds, dx))
            def _():
                cross_copy(i, slot).wait_send()

        for d in range(1, groups):
            peer_copy(d, slot).wait_recv()
            tile_copy(0, d, slot).wait_recv()
        for d in range(groups):
            @pl.when(s > 0)
            def _():
                tile_copy(1, d, slot).wait_recv()

            @pl.when(s < sections - 1)
            def _():
                tile_copy(-1, d, slot).wait_recv()
        inputs_low = solve(k, slot)

        acc = jnp.zeros((8, LANES), F32)
        for q in range(PLANES + 1, -1, -1):
            drive(q, inputs_low)
            if q < PLANES:
                acc = update(q, acc)
            if q < PLANES - 1:
                apply(q + 1)
            if q == PLANES - 2:
                apply_outside(1)

                @pl.when(k < ITERS - 1)
                def _():
                    start_cross(early, 1 - slot)
        apply(0)
        apply_outside(0)
        record_primal(k, acc)

        for d in range(1, groups):
            peer_copy(d, slot).wait_send()
            tile_copy(0, d, slot).wait_send()
        for d in range(groups):
            @pl.when(s < sections - 1)
            def _():
                tile_copy(1, d, slot).wait_send()

            @pl.when(s > 0)
            def _():
                tile_copy(-1, d, slot).wait_send()
        return carry

    lax.fori_loop(1, ITERS, iteration, 0)

    def first_copy(e):
        return pltpu.make_async_remote_copy(
            src_ref=hist, dst_ref=first_in.at[e - 1], send_sem=hist_send.at[e - 1], recv_sem=hist_recv.at[e - 1],
            device_id=pair_peer(e), device_id_type=MESH)

    def second_copy(e):
        i = pair_count - 2 + e
        return pltpu.make_async_remote_copy(
            src_ref=second, dst_ref=second_in.at[e - 1], send_sem=hist_send.at[i], recv_sem=hist_recv.at[i],
            device_id=column_peer(e), device_id_type=MESH)

    for e in range(1, pair_count):
        first_copy(e).start()

    for p in range(PLANES):
        for j in range(CHUNKS):
            ref_ref[j, pl.ds(p, ROWS, stride=PLANES), :] = S[p + 1, j, 8:32, :]
            weight_ref[j, pl.ds(p, ROWS, stride=PLANES), :] = dual[p, j]
    stores = [
        pltpu.make_async_copy(ref_ref, states_out, flat_sem.at[0, 0]),
        pltpu.make_async_copy(weight_ref, dual_out, flat_sem.at[1, 0]),
    ]
    for copy in stores:
        copy.start()
    boxed_out[...] = boxed[0:ROWS]

    for e in range(1, pair_count):
        first_copy(e).wait()
    total = hist[...]
    for e in range(1, pair_count):
        total = total + first_in[e - 1]
    second[...] = total
    for e in range(1, columns):
        second_copy(e).start()
    for e in range(1, columns):
        second_copy(e).wait()
    for e in range(1, columns):
        total = total + second_in[e - 1]
    row = lax.broadcasted_iota(jnp.int32, (8, LANES), 0)
    cells = float(ROWS * sections * GX * GY * GZ)
    inputs_count = float(ROWS * sections * WIDTH * groups)
    for copy in stores:
        copy.wait()
    hist_out[...] = jnp.sqrt(jnp.where(row == 0, total * (1.0 / cells), total * (1.0 / inputs_count)) + epsilon)


def deliver(states, boxed, dual_vars, record, states_out, boxed_out, dual_out, record_out, a, b, sem):
    loads, stores = [], []
    for i, (source, held, target) in enumerate(((states, a, states_out), (dual_vars, b, dual_out))):
        for j in range(CHUNKS):
            cells = pl.ds(j * LANES, LANES)
            loads.append(pltpu.make_async_copy(source.at[j], held.at[j], sem.at[i, j]))
            stores.append(pltpu.make_async_copy(held.at[j], target.at[:, cells], sem.at[2 + i, j]))
    for copy in loads:
        copy.start()
    boxed_out[...] = boxed[...]
    record_out[...] = record[0:2, 0:ITERS]
    for load, store in zip(loads, stores):
        load.wait()
        store.start()
    for copy in stores:
        copy.wait()


def solution(mesh):
    sections, groups = mesh.shape["section"], mesh.shape["state"]
    columns = sections // 2

    def local(initial_state, state_ref, state_weight, input_matrix, kkt_inverse, input_bound):
        vmem = pl.BlockSpec(memory_space=pltpu.VMEM)
        any_space = pl.BlockSpec(memory_space=pl.ANY)
        flat = (ROWS * PLANES, PLANE)
        chunked = (CHUNKS, ROWS * PLANES, LANES)
        V = pltpu.VMEM
        DMA = pltpu.SemaphoreType.DMA
        message_count = 10 + groups - 1 + 3 * groups
        compact = (CHUNKS, LANES)
        states, boxed, dual_vars, record = pl.pallas_call(
            functools.partial(kernel, sections, groups),
            out_shape=(
                jax.ShapeDtypeStruct(chunked, F32),
                jax.ShapeDtypeStruct((ROWS, WIDTH), F32),
                jax.ShapeDtypeStruct(chunked, F32),
                jax.ShapeDtypeStruct((8, LANES), F32),
            ),
            in_specs=[vmem, any_space, any_space, any_space, any_space, vmem],
            out_specs=(any_space, vmem, any_space, vmem),
            scratch_shapes=[
                V((CHUNKS, ROWS * PLANES, LANES), F32),
                V((CHUNKS, ROWS * PLANES, LANES), F32),
                V((WIDTH, WIDTH), F32),
                V((PLANES + 2, PLANE, WIDTH), BF16),
                V((PLANES + 2, WIDTH, PLANE), BF16),
                V((PLANES + 2, CHUNKS, 40, LANES), F32),
                V((PLANES, CHUNKS, 40, LANES), F32),
                V((PLANES + 2, CHUNKS, 32, LANES), F32),
                V((PLANES + 2, CHUNKS, 32, LANES), F32),
                V((PLANES, CHUNKS, ROWS, LANES), F32),
                V((PLANES, CHUNKS, ROWS, LANES), F32),
                V((PLANES, CHUNKS, ROWS, LANES), F32),
                V((32, (PLANES + 2) * PLANE), BF16),
                V((2, 2, 16, 2 * FOLD), BF16),
                V((PLANES + 2, *compact), F32),
                V((PLANES, *compact), F32),
                V((2, PLANES, *compact), F32),
                V((2, *compact), F32),
                V((2, *compact), F32),
                V((2, PLANES, *compact), F32),
                V((2, *compact), F32),
                V((2, *compact), F32),
                V((2, 16, 2 * FOLD), BF16),
                V((2, 2, 2, *compact), F32),
                V((32, WIDTH), F32),
                V((16, WIDTH + WIDTH // 2), BF16),
                V((2, groups - 1, 16, WIDTH + WIDTH // 2), BF16),
                V((2, PLANES, PLANE), F32),
                V(compact, F32),
                V((2, groups, *compact), F32),
                V((2, groups - 1, *compact), F32),
                V((2, groups, *compact), F32),
                V((WIDTH, WIDTH), BF16),
                V((WIDTH, WIDTH), BF16),
                V((32, WIDTH), F32),
                V((32, WIDTH), F32),
                V((32, WIDTH), F32),
                V(compact, F32),
                V((2 * groups - 1, *compact), F32),
                V(compact, F32),
                V((max(columns - 1, 1), *compact), F32),
                DMA((PLANES + 1,)),
                DMA((2, CHUNKS)),
                DMA((2, BLOCKS)),
                DMA((2, BLOCKS)),
                DMA((2, BLOCKS)),
                DMA((2, BLOCKS)),
                DMA((2,)),
                DMA((2,)),
                DMA((message_count,)),
                DMA((2, message_count)),
                DMA((2 * groups + columns,)),
                DMA((2 * groups + columns,)),
            ],
            compiler_params=pltpu.CompilerParams(
                collective_id=0, has_side_effects=True, vmem_limit_bytes=64000 * 1024),
        )(
            initial_state,
            state_ref.reshape(flat),
            state_weight.reshape(flat),
            input_matrix,
            kkt_inverse,
            input_bound.reshape(1, WIDTH),
        )
        states, boxed, dual_vars, record = pl.pallas_call(
            deliver,
            out_shape=(
                jax.ShapeDtypeStruct(flat, F32),
                jax.ShapeDtypeStruct((ROWS, WIDTH), F32),
                jax.ShapeDtypeStruct(flat, F32),
                jax.ShapeDtypeStruct((2, ITERS), F32),
            ),
            in_specs=[any_space, vmem, any_space, vmem],
            out_specs=(any_space, vmem, any_space, vmem),
            scratch_shapes=[V(chunked, F32), V(chunked, F32), DMA((4, CHUNKS))],
        )(states, boxed, dual_vars, record)
        return (states.reshape(state_ref.shape), boxed, dual_vars.reshape(state_ref.shape), record.T)

    return jax.shard_map(
        local,
        mesh=mesh,
        in_specs=(
            P("state", None),
            P("section", "state", None),
            P("section", "state", None),
            P("state", None, None),
            P(),
            P(),
        ),
        out_specs=(P("section", "state", None), P("section", None), P("section", "state", None), P()),
        check_vma=False,
    )
```
